32 devices in a mesh: farcp: 2 (over x), nearcp: 4 (over y, core), model: 4 (over z).
Axes of the slice: x: 2, y: 2, z: 4, core: 2. Of those that a mesh axis runs over, the one named last changes fastest.
Arguments:
- raw_keys: bfloat16 [8, 8192, 8, 128], P(None, ('farcp', 'nearcp'), 'model'), may hold values from -6 to 6
- raw_values: bfloat16 [8, 8192, 8, 128], P(None, ('farcp', 'nearcp'), 'model'), may hold values from -6 to 6
- turn_angle: float32 [8192, 64], replicated, may hold values from -3.140625 to 3.140625
- key_gain: float32 [128], replicated, may hold values from 0.25 to 1.75
Outputs:
- stored_keys: bfloat16 [8, 8192, 8, 128], P(('farcp', 'nearcp'), None, 'model')
- stored_values: bfloat16 [8, 8192, 8, 128], P(('farcp', 'nearcp'), None, 'model')
- key_scale: float32 [8, 8, 128], P(('farcp', 'nearcp'), 'model')
The draws below stay inside these ranges and needn't reach their ends.
All inputs are finite; a program needn't handle non-finite values. Where the reference program divides by a largest or mean magnitude, that divisor is 1e-20 or more.
Results may differ from the reference program's by a relative error of at most 0.001.
Values may be sent and summed in bfloat16 or wider, within the bound.
A program may use at most 192 MiB of HBM per device.

```python
import jax
import jax.numpy as jnp
from jax import lax

BATCH = 8
LENGTH = 8192
KV_HEADS = 8
HEAD_SIZE = 128
HALF_HEAD = 64


def steps_of(rng, extent, cuts, low, largest):
    loudness = 1.0
    for dim, shards_of in cuts:
        draws = jax.random.uniform(jax.random.fold_in(jax.random.fold_in(rng, 6), dim), (shards_of,), jnp.float32, low / len(cuts), largest / len(cuts))
        loudness = loudness * jnp.repeat(jnp.exp(draws), extent[dim] // shards_of).reshape((-1,) + (1,) * (len(extent) - 1 - dim))
    return loudness


def gaussian(stream_key, extent, scale, reach, pieces=(), dtype=jnp.bfloat16):
    array = scale * jax.random.normal(stream_key, extent, jnp.float32)
    if pieces:
        array = array * steps_of(stream_key, extent, pieces, -0.22, 0.18)
    return jnp.clip(array, -reach, reach).astype(dtype)


def setup_inputs(seed: int = 0) -> dict:
    keys = jax.random.split(jax.random.key(seed), 5)
    return {
        "raw_keys": gaussian(keys[0], (BATCH, LENGTH, KV_HEADS, HEAD_SIZE), 1.0, 6.0, ((1, 8), (2, 4))),
        "raw_values": gaussian(keys[1], (BATCH, LENGTH, KV_HEADS, HEAD_SIZE), 1.0, 6.0, ((1, 8), (2, 4))),
        "turn_angle": jnp.clip(jax.random.uniform(keys[2], (LENGTH, HALF_HEAD), jnp.float32, -3.140625, 3.140625), -3.140625, 3.140625),
        "key_gain": jnp.clip(1.0 + 0.15 * jax.random.normal(keys[3], (HEAD_SIZE,), jnp.float32), 0.25, 1.75),
    }


def apply_rotary(vectors, angle):
    half = vectors.shape[-1] // 2
    cosine, sine = (jnp.cos(angle)[None, :, None, :], jnp.sin(angle)[None, :, None, :])
    first, second = (vectors[..., :half], vectors[..., half:])
    return jnp.concatenate([first * cosine - second * sine, second * cosine + first * sine], axis=-1)

def scale_rows(vectors, row_gain):
    return vectors * lax.rsqrt(lax.optimization_barrier(jnp.mean(vectors * vectors, axis=-1, keepdims=True)) + 1e-06) * row_gain

def prepare_keys(plain_keys, angle, key_gain):
    wide_keys = plain_keys.astype(jnp.float32)
    wide_keys = scale_rows(wide_keys, key_gain)
    return apply_rotary(wide_keys, angle)

def reference(raw_keys, raw_values, turn_angle, key_gain):
    turned_keys = prepare_keys(raw_keys, turn_angle, key_gain)
    key_scale = lax.optimization_barrier(jnp.max(jnp.abs(turned_keys), axis=1))
    narrow_keys = (turned_keys / key_scale[:, None]).astype(jnp.bfloat16)
    stored_keys = narrow_keys
    stored_values = raw_values
    return (stored_keys, stored_values, key_scale)
```

```python
import functools

import jax
import jax.numpy as jnp
from jax import lax
from jax.experimental import pallas as pl
from jax.experimental.pallas import tpu as pltpu
from jax.sharding import PartitionSpec as P

FAR, NEAR = "farcp", "nearcp"
MESH_ID = pl.DeviceIdType.MESH
TILE = 256
LATE = 3
TAIL_VMEM = 51 * 1024 * 1024
WRITES = 4
LANES = 128


def step_kinds(far_size, near_size):
    kinds = {"both": [], "first": [], "second": [], "same": []}
    for step in range(1, far_size * near_size):
        far, chip = step // near_size > 0, step % near_size > 1
        kinds["both" if far and chip else "first" if far else "second" if chip else "same"].append(step)
    return kinds


def mixed(*lists):
    order = []
    for turn in range(max(map(len, lists))):
        order += [steps[turn] for steps in lists if turn < len(steps)]
    return order


def late_rows(rows):
    return rows * LATE // (4 * LANES) * LANES


def exchange_plan(far_size, near_size, rows):
    kinds = step_kinds(far_size, near_size)
    both, first, second, same = (kinds[kind] for kind in ("both", "first", "second", "same"))
    late = late_rows(rows)
    early = rows - late

    def straight(steps, parity):
        return [step for step in steps if step % 2 == parity]

    def whole(which, steps):
        return [(which, step, 0, rows) for step in steps]

    crossing = mixed(straight(first, 1), straight(second, 1), straight(both, 1)) + straight(same, 1)
    part = [(1, step, 0, early) for step in straight(both, 0)] if early else []
    rest = [(1, step, early, late) for step in straight(both, 0)]
    even = whole(0, mixed(both, first, second) + same) + part + whole(1, crossing)
    odd = whole(0, mixed(first, both, second) + same) + whole(1, crossing) + part
    odd += whole(1, mixed(straight(first, 0), straight(second, 0))) + rest
    tail = [(step, 0, rows) for step in mixed(straight(first, 0), straight(second, 0))]
    tail += [(step, early, late) for step in straight(both, 0)]
    return even, odd, tail


def position(near_size):
    return lax.axis_index(FAR) * near_size + lax.axis_index(NEAR)


def device(index, near_size):
    return {FAR: index // near_size, NEAR: index % near_size}


def greet(barrier, me, near_size, steps):
    for step in steps:
        pl.semaphore_signal(
            barrier, inc=1, device_id=device(me ^ step, near_size), device_id_type=MESH_ID
        )
    pl.semaphore_wait(barrier, len(steps))


def exchange_kernel(
    far_size, near_size, heads, keys_ref, values_ref, turn_ref, plain_gain_ref,
    out_keys, out_values, out_scale,
    angle_ref, gain_ref, landed, cos_table, sin_table, turned, send_sem, recv_sem, local_sem,
):
    me = position(near_size)
    rows = keys_ref.shape[1]
    total_rows = landed.shape[0]
    half = angle_ref.shape[0]
    devices = far_size * near_size
    even, odd, _ = exchange_plan(far_size, near_size, rows)
    slot = {copy: i for i, copy in enumerate(dict.fromkeys(even + odd))}

    angles = pltpu.make_async_copy(turn_ref, angle_ref, local_sem.at[2])
    gains = pltpu.make_async_copy(plain_gain_ref, gain_ref, local_sem.at[3])
    own = [
        pltpu.make_async_copy(src.at[me], dst.at[pl.ds(me * rows, rows)], local_sem.at[i])
        for i, (src, dst) in enumerate(((keys_ref, landed), (values_ref, out_values)))
    ]

    def remote(copy):
        which, step, offset, size = copy
        src, dst = ((keys_ref, landed), (values_ref, out_values))[which]
        return pltpu.make_async_remote_copy(
            src_ref=src.at[me ^ step, pl.ds(offset, size)],
            dst_ref=dst.at[pl.ds(me * rows + offset, size)],
            send_sem=send_sem.at[slot[copy]],
            recv_sem=recv_sem.at[slot[copy]],
            device_id=device(me ^ step, near_size),
            device_id_type=MESH_ID,
        )

    greet(pltpu.get_barrier_semaphore(), me, near_size, range(1, devices))
    for parity, copies in enumerate((even, odd)):

        @pl.when(me % 2 == parity)
        def _():
            for copy in copies:
                remote(copy).start()

    for copy in (angles, gains, *own):
        copy.start()
    angles.wait()
    gains.wait()
    gain = gain_ref[...]
    other_gain = pltpu.roll(gain, half, 1)

    def fill(block, carry):
        angle = angle_ref[:, pl.ds(pl.multiple_of(block * LANES, LANES), LANES)]
        cosine, sine = jnp.cos(angle), jnp.sin(angle)
        cosine = jnp.concatenate([cosine, cosine], axis=0).T * gain
        sine = jnp.concatenate([-sine, sine], axis=0).T * other_gain
        for head in range(heads):
            place = pl.ds(block * (LANES * heads) + head, LANES, stride=heads)
            cos_table[place, :] = cosine
            sin_table[place, :] = sine
        return carry

    lax.fori_loop(0, total_rows // (heads * LANES), fill, 0)

    def prepare(owner, largest):
        def body(i, largest):
            place = pl.ds(pl.multiple_of(owner * rows + i * TILE, TILE), TILE)
            x = landed[place, :].astype(jnp.float32)
            mean = jnp.sum(x * x, axis=-1, keepdims=True) * (1.0 / x.shape[-1])
            x = x * lax.rsqrt(mean + 1e-06)
            t = x * cos_table[place, :] + pltpu.roll(x, half, 1) * sin_table[place, :]
            turned[place, :] = t
            return jnp.maximum(largest, jnp.max(jnp.abs(t).reshape(TILE // 8, 8, LANES), axis=0))

        return lax.fori_loop(0, rows // TILE, body, largest)

    largest = jnp.zeros((8, LANES), jnp.float32)
    own[0].wait()
    largest = prepare(me, largest)
    for copy in even[devices - 2 :: -1]:
        remote(copy).wait_recv()
        largest = prepare(me ^ copy[1], largest)

    head_of = lax.broadcasted_iota(jnp.int32, (8, LANES), 0) % heads
    scale = jnp.zeros((8, LANES), jnp.float32)
    for head in range(heads):
        top = jnp.max(jnp.where(head_of == head, largest, 0.0), axis=0, keepdims=True)
        out_scale[pl.ds(head, 1), :] = top
        scale = jnp.where(head_of == head, top, scale)
    inverse = (1.0 / scale)[None]

    def narrow(i, carry):
        place = pl.ds(pl.multiple_of(i * TILE, TILE), TILE)
        t = turned[place, :].reshape(TILE // 8, 8, LANES) * inverse
        out_keys[place, :] = t.reshape(TILE, LANES).astype(out_keys.dtype)
        return carry

    lax.fori_loop(0, total_rows // TILE, narrow, 0)

    own[1].wait()
    for parity, mine, theirs in ((0, even, odd), (1, odd, even)):

        @pl.when(me % 2 == parity)
        def _():
            for copies, crossed in ((mine, 0), (theirs, 1)):
                for copy in copies:
                    if copy[0] == 1 and copy[1] % 2 == crossed:
                        remote(copy).wait_recv()
            for copy in mine:
                remote(copy).wait_send()


def tail_kernel(far_size, near_size, values_ref, after_ref, out_ref, send_sem, recv_sem):
    me = position(near_size)
    rows = values_ref.shape[1]
    plan = exchange_plan(far_size, near_size, rows)[2]

    @pl.when(me % 2 == 0)
    def _():
        greet(pltpu.get_barrier_semaphore(), me, near_size, [step for step, _, _ in plan])
        copies, place = [], 0
        for i, (step, offset, size) in enumerate(plan):
            copies.append(
                pltpu.make_async_remote_copy(
                    src_ref=values_ref.at[me ^ step, pl.ds(offset, size)],
                    dst_ref=out_ref.at[pl.ds(place, size)],
                    send_sem=send_sem.at[i],
                    recv_sem=recv_sem.at[i],
                    device_id=device(me ^ step, near_size),
                    device_id_type=MESH_ID,
                )
            )
            place += size
        for copy in copies:
            copy.start()
        for copy in copies:
            copy.wait_recv()
        for copy in copies:
            copy.wait_send()


def place_kernel(
    keys_ref, values_ref, scale_ref, out_keys, out_values, out_scale, after_ref, sem
):
    part = keys_ref.shape[0] // WRITES
    copies = [
        pltpu.make_async_copy(scale_ref, dst, sem.at[2, i]) for i, dst in enumerate((out_scale, after_ref))
    ]
    for i, (src, dst) in enumerate(((keys_ref, out_keys), (values_ref, out_values))):
        for j in range(WRITES):
            place = pl.ds(j * part, part)
            copies.append(pltpu.make_async_copy(src.at[place], dst.at[place], sem.at[i, j]))
    for copy in copies:
        copy.start()
    for copy in copies:
        copy.wait()


def place_tail_kernel(far_size, near_size, rows, values_ref, late_ref, out_ref, sem):
    me = position(near_size)

    @pl.when(me % 2 == 0)
    def _():
        copies, place = [], 0
        for i, (step, offset, size) in enumerate(exchange_plan(far_size, near_size, rows)[2]):
            copies.append(
                pltpu.make_async_copy(
                    late_ref.at[pl.ds(place, size)],
                    out_ref.at[pl.ds((me ^ step) * rows + offset, size)],
                    sem.at[i],
                )
            )
            place += size
        for copy in copies:
            copy.start()
        for copy in copies:
            copy.wait()


def local(far_size, near_size, raw_keys, raw_values, turn_angle, key_gain):
    sequences, positions, heads, size = raw_keys.shape
    devices = far_size * near_size
    rows = positions * heads
    total = rows * devices
    flat = (sequences, rows, size)
    even, odd, tail = exchange_plan(far_size, near_size, rows)
    raw_values = raw_values.reshape(flat)
    whole = pltpu.VMEM((total, size), raw_keys.dtype)
    keys, values, scale = pl.pallas_call(
        functools.partial(exchange_kernel, far_size, near_size, heads),
        out_shape=(whole, whole, pltpu.VMEM((heads, size), jnp.float32)),
        in_specs=[
            pl.BlockSpec(memory_space=pl.ANY),
            pl.BlockSpec(memory_space=pl.ANY),
            pl.BlockSpec(memory_space=pl.ANY),
            pl.BlockSpec(memory_space=pl.ANY),
        ],
        out_specs=(
            pl.BlockSpec(memory_space=pltpu.VMEM),
            pl.BlockSpec(memory_space=pltpu.VMEM),
            pl.BlockSpec(memory_space=pltpu.VMEM),
        ),
        scratch_shapes=[
            pltpu.VMEM((size // 2, total // heads), jnp.float32),
            pltpu.VMEM((1, size), jnp.float32),
            pltpu.VMEM((total, size), raw_keys.dtype),
            pltpu.VMEM((total, size), jnp.float32),
            pltpu.VMEM((total, size), jnp.float32),
            pltpu.VMEM((total, size), jnp.float32),
            pltpu.SemaphoreType.DMA((len(set(even + odd)),)),
            pltpu.SemaphoreType.DMA((len(set(even + odd)),)),
            pltpu.SemaphoreType.DMA((4,)),
        ],
        compiler_params=pltpu.CompilerParams(
            collective_id=0, has_side_effects=True, vmem_limit_bytes=48 * 1024 * 1024
        ),
        name="exchange",
    )(raw_keys.reshape(flat), raw_values, turn_angle.T, key_gain.reshape(1, size))
    out = jax.ShapeDtypeStruct((total, size), raw_keys.dtype)
    in_vmem = pl.BlockSpec(memory_space=pltpu.VMEM)
    anywhere = pl.BlockSpec(memory_space=pl.ANY)
    keys, values, scale, after = pl.pallas_call(
        place_kernel,
        out_shape=(
            out, out, jax.ShapeDtypeStruct((heads, size), jnp.float32),
            jax.ShapeDtypeStruct((heads, size), jnp.float32),
        ),
        in_specs=[in_vmem] * 3,
        out_specs=[anywhere] * 4,
        scratch_shapes=[pltpu.SemaphoreType.DMA((3, WRITES))],
        compiler_params=pltpu.CompilerParams(vmem_limit_bytes=12 * 1024 * 1024),
        name="place",
    )(keys, values, scale)
    late = pl.pallas_call(
        functools.partial(tail_kernel, far_size, near_size),
        out_shape=pltpu.VMEM((sum(copy[2] for copy in tail), size), raw_keys.dtype),
        in_specs=[anywhere, anywhere],
        out_specs=in_vmem,
        scratch_shapes=[pltpu.SemaphoreType.DMA((len(tail),))] * 2,
        compiler_params=pltpu.CompilerParams(
            collective_id=1, has_side_effects=True, vmem_limit_bytes=TAIL_VMEM
        ),
        name="tail",
    )(raw_values, after)
    values = pl.pallas_call(
        functools.partial(place_tail_kernel, far_size, near_size, rows),
        out_shape=out,
        in_specs=[anywhere, in_vmem],
        out_specs=anywhere,
        input_output_aliases={0: 0},
        scratch_shapes=[pltpu.SemaphoreType.DMA((len(tail),))],
        compiler_params=pltpu.CompilerParams(vmem_limit_bytes=12 * 1024 * 1024),
        name="place_tail",
    )(values, late)
    full = (1, positions * devices, heads, size)
    return keys.reshape(full), values.reshape(full), scale.reshape(1, heads, size)


def solution(mesh):
    in_specs = (
        P(None, (FAR, NEAR), "model", None),
        P(None, (FAR, NEAR), "model", None),
        P(),
        P(),
    )
    out_specs = (
        P((FAR, NEAR), None, "model", None),
        P((FAR, NEAR), None, "model", None),
        P((FAR, NEAR), "model", None),
    )
    body = functools.partial(local, mesh.shape[FAR], mesh.shape[NEAR])
    return jax.shard_map(body, mesh=mesh, in_specs=in_specs, out_specs=out_specs, check_vma=False)
```

```python
import functools

import jax
import jax.numpy as jnp
from jax import lax
from jax.experimental import pallas as pl
from jax.experimental.pallas import tpu as pltpu
from jax.sharding import PartitionSpec as P

FAR, NEAR = "farcp", "nearcp"
MESH_ID = pl.DeviceIdType.MESH
TILE = 256
LATE = 14
LAST = 3
TAIL_VMEM = 51 * 1024 * 1024
WRITES = 4
LANES = 128


def step_kinds(far_size, near_size):
    kinds = {"both": [], "first": [], "second": [], "same": []}
    for step in range(1, far_size * near_size):
        far, chip = step // near_size > 0, step % near_size > 1
        kinds["both" if far and chip else "first" if far else "second" if chip else "same"].append(step)
    return kinds


def mixed(*lists):
    order = []
    for turn in range(max(map(len, lists))):
        order += [steps[turn] for steps in lists if turn < len(steps)]
    return order


def late_rows(rows):
    return rows * LATE // (16 * LANES) * LANES


def exchange_plan(far_size, near_size, rows):
    kinds = step_kinds(far_size, near_size)
    both, first, second, same = (kinds[kind] for kind in ("both", "first", "second", "same"))
    late = late_rows(rows)
    early = rows - late

    def straight(steps, parity):
        return [step for step in steps if step % 2 == parity]

    def whole(which, steps):
        return [(which, step, 0, rows) for step in steps]

    crossing = mixed(straight(first, 1), straight(second, 1), straight(both, 1)) + straight(same, 1)
    part = [(1, step, 0, early) for step in straight(both, 0)] if early else []
    rest = [(1, step, early, late) for step in straight(both, 0)]
    last = LAST * LANES
    even = whole(0, second + mixed(both, first) + same) + part
    even += [(1, step, 0, last) for step in straight(second, 0)] + whole(1, crossing)
    odd = whole(0, second + mixed(first, both) + same) + whole(1, crossing) + part
    odd += whole(1, mixed(straight(first, 0), straight(second, 0))) + rest
    corner = mixed(
        [(step, 0, rows - last) for step in straight(first, 0)],
        [(step, last, rows - last) for step in straight(second, 0)],
    )
    corner += [(step, early, late) for step in straight(both, 0)]
    return even, odd, corner + [(step, rows - last, last) for step in straight(first, 0)]


def position(near_size):
    return lax.axis_index(FAR) * near_size + lax.axis_index(NEAR)


def device(index, near_size):
    return {FAR: index // near_size, NEAR: index % near_size}


def signal(semaphore, index, near_size):
    pl.semaphore_signal(
        semaphore, inc=1, device_id=device(index, near_size), device_id_type=MESH_ID
    )


def greet(barrier, me, near_size, steps):
    for step in steps:
        signal(barrier, me ^ step, near_size)
    pl.semaphore_wait(barrier, len(steps))


def greet_upwards(barrier, ready, me, near_size, steps):
    below = 0
    for step in steps:
        below += jnp.where((me & step) == step, 1, 0)
        pl.when((me & step) == 0)(functools.partial(signal, barrier, me ^ step, near_size))
    pl.when(me > 0)(functools.partial(pl.semaphore_wait, barrier, below))
    for step in steps:
        answer = functools.partial(signal, ready.at[step], me ^ step, near_size)
        pl.when((me & step) == step)(answer)


def exchange_kernel(
    far_size, near_size, heads, keys_ref, values_ref, turn_ref, plain_gain_ref,
    out_keys, out_values, out_scale,
    angle_ref, gain_ref, landed, cos_table, sin_table, turned, send_sem, recv_sem, ready, local_sem,
):
    me = position(near_size)
    rows = keys_ref.shape[1]
    total_rows = landed.shape[0]
    half = angle_ref.shape[0]
    devices = far_size * near_size
    even, odd, _ = exchange_plan(far_size, near_size, rows)
    slot = {copy: i for i, copy in enumerate(dict.fromkeys(even + odd))}

    angles = pltpu.make_async_copy(turn_ref, angle_ref, local_sem.at[2])
    gains = pltpu.make_async_copy(plain_gain_ref, gain_ref, local_sem.at[3])
    own = [
        pltpu.make_async_copy(src.at[me], dst.at[pl.ds(me * rows, rows)], local_sem.at[i])
        for i, (src, dst) in enumerate(((keys_ref, landed), (values_ref, out_values)))
    ]

    def remote(copy):
        which, step, offset, size = copy
        src, dst = ((keys_ref, landed), (values_ref, out_values))[which]
        return pltpu.make_async_remote_copy(
            src_ref=src.at[me ^ step, pl.ds(offset, size)],
            dst_ref=dst.at[pl.ds(me * rows + offset, size)],
            send_sem=send_sem.at[slot[copy]],
            recv_sem=recv_sem.at[slot[copy]],
            device_id=device(me ^ step, near_size),
            device_id_type=MESH_ID,
        )

    kinds = step_kinds(far_size, near_size)
    stages = (kinds["second"] + kinds["same"], kinds["first"], kinds["both"])
    greet_upwards(pltpu.get_barrier_semaphore(), ready, me, near_size, sum(stages, []))

    def wait_ready(steps):
        for step in steps:
            wait = functools.partial(pl.semaphore_wait, ready.at[step], 1)
            pl.when((me & step) == 0)(wait)

    wait_ready(stages[0])
    for step in kinds["second"]:
        remote((0, step, 0, rows)).start()
    for parity, copies in enumerate((even, odd)):

        @pl.when(me % 2 == parity)
        def _():
            waited = 1
            for copy in copies[len(kinds["second"]) :]:
                stage = [i for i, steps in enumerate(stages) if copy[1] in steps][0]
                for i in range(waited, stage + 1):
                    wait_ready(stages[i])
                waited = max(waited, stage + 1)
                remote(copy).start()

    for copy in (angles, gains, *own):
        copy.start()
    angles.wait()
    gains.wait()
    gain = gain_ref[...]
    other_gain = pltpu.roll(gain, half, 1)

    def fill(block, carry):
        angle = angle_ref[:, pl.ds(pl.multiple_of(block * LANES, LANES), LANES)]
        cosine, sine = jnp.cos(angle), jnp.sin(angle)
        cosine = jnp.concatenate([cosine, cosine], axis=0).T * gain
        sine = jnp.concatenate([-sine, sine], axis=0).T * other_gain
        for head in range(heads):
            place = pl.ds(block * (LANES * heads) + head, LANES, stride=heads)
            cos_table[place, :] = cosine
            sin_table[place, :] = sine
        return carry

    lax.fori_loop(0, total_rows // (heads * LANES), fill, 0)

    def prepare(owner, largest):
        def body(i, largest):
            place = pl.ds(pl.multiple_of(owner * rows + i * TILE, TILE), TILE)
            x = landed[place, :].astype(jnp.float32)
            mean = jnp.sum(x * x, axis=-1, keepdims=True) * (1.0 / x.shape[-1])
            x = x * lax.rsqrt(mean + 1e-06)
            t = x * cos_table[place, :] + pltpu.roll(x, half, 1) * sin_table[place, :]
            turned[place, :] = t
            return jnp.maximum(largest, jnp.max(jnp.abs(t).reshape(TILE // 8, 8, LANES), axis=0))

        return lax.fori_loop(0, rows // TILE, body, largest)

    largest = jnp.zeros((8, LANES), jnp.float32)
    own[0].wait()
    largest = prepare(me, largest)
    for copy in even[devices - 2 :: -1]:
        remote(copy).wait_recv()
        largest = prepare(me ^ copy[1], largest)

    head_of = lax.broadcasted_iota(jnp.int32, (8, LANES), 0) % heads
    scale = jnp.zeros((8, LANES), jnp.float32)
    for head in range(heads):
        top = jnp.max(jnp.where(head_of == head, largest, 0.0), axis=0, keepdims=True)
        out_scale[pl.ds(head, 1), :] = top
        scale = jnp.where(head_of == head, top, scale)
    inverse = (1.0 / scale)[None]

    def narrow(i, carry):
        place = pl.ds(pl.multiple_of(i * TILE, TILE), TILE)
        t = turned[place, :].reshape(TILE // 8, 8, LANES) * inverse
        out_keys[place, :] = t.reshape(TILE, LANES).astype(out_keys.dtype)
        return carry

    lax.fori_loop(0, total_rows // TILE, narrow, 0)

    own[1].wait()
    for parity, mine, theirs in ((0, even, odd), (1, odd, even)):

        @pl.when(me % 2 == parity)
        def _():
            for copies, crossed in ((mine, 0), (theirs, 1)):
                for copy in copies:
                    if copy[0] == 1 and copy[1] % 2 == crossed:
                        remote(copy).wait_recv()
            for copy in mine:
                remote(copy).wait_send()


def tail_kernel(far_size, near_size, values_ref, after_ref, out_ref, send_sem, recv_sem):
    me = position(near_size)
    rows = values_ref.shape[1]
    plan = exchange_plan(far_size, near_size, rows)[2]

    @pl.when(me % 2 == 0)
    def _():
        greet(pltpu.get_barrier_semaphore(), me, near_size, sorted({step for step, _, _ in plan}))
        copies, place = {}, 0
        for i, (step, offset, size) in enumerate(plan):
            copies[step, offset] = (
                pltpu.make_async_remote_copy(
                    src_ref=values_ref.at[me ^ step, pl.ds(offset, size)],
                    dst_ref=out_ref.at[pl.ds(place, size)],
                    send_sem=send_sem.at[i],
                    recv_sem=recv_sem.at[i],
                    device_id=device(me ^ step, near_size),
                    device_id_type=MESH_ID,
                )
            )
            place += size
        kinds = step_kinds(far_size, near_size)
        inner = [copy for copy in plan if copy[0] not in kinds["both"]]
        outer = [copy for copy in plan if copy[0] in kinds["both"]]
        bent = me == near_size
        for order, here in ((inner + outer, bent), (plan, ~bent)):

            @pl.when(here)
            def _():
                for step, offset, _ in order:
                    copies[step, offset].start()

        for copy in copies.values():
            copy.wait_recv()
        for copy in copies.values():
            copy.wait_send()


def place_kernel(
    keys_ref, values_ref, scale_ref, out_keys, out_values, out_scale, after_ref, sem
):
    part = keys_ref.shape[0] // WRITES
    copies = [
        pltpu.make_async_copy(scale_ref, dst, sem.at[2, i]) for i, dst in enumerate((out_scale, after_ref))
    ]
    for i, (src, dst) in enumerate(((keys_ref, out_keys), (values_ref, out_values))):
        for j in range(WRITES):
            place = pl.ds(j * part, part)
            copies.append(pltpu.make_async_copy(src.at[place], dst.at[place], sem.at[i, j]))
    for copy in copies:
        copy.start()
    for copy in copies:
        copy.wait()


def place_tail_kernel(far_size, near_size, rows, values_ref, late_ref, out_ref, sem):
    me = position(near_size)

    @pl.when(me % 2 == 0)
    def _():
        copies, place = [], 0
        for i, (step, offset, size) in enumerate(exchange_plan(far_size, near_size, rows)[2]):
            copies.append(
                pltpu.make_async_copy(
                    late_ref.at[pl.ds(place, size)],
                    out_ref.at[pl.ds((me ^ step) * rows + offset, size)],
                    sem.at[i],
                )
            )
            place += size
        for copy in copies:
            copy.start()
        for copy in copies:
            copy.wait()


def local(far_size, near_size, raw_keys, raw_values, turn_angle, key_gain):
    sequences, positions, heads, size = raw_keys.shape
    devices = far_size * near_size
    rows = positions * heads
    total = rows * devices
    flat = (sequences, rows, size)
    even, odd, tail = exchange_plan(far_size, near_size, rows)
    raw_values = raw_values.reshape(flat)
    whole = pltpu.VMEM((total, size), raw_keys.dtype)
    keys, values, scale = pl.pallas_call(
        functools.partial(exchange_kernel, far_size, near_size, heads),
        out_shape=(whole, whole, pltpu.VMEM((heads, size), jnp.float32)),
        in_specs=[
            pl.BlockSpec(memory_space=pl.ANY),
            pl.BlockSpec(memory_space=pl.ANY),
            pl.BlockSpec(memory_space=pl.ANY),
            pl.BlockSpec(memory_space=pl.ANY),
        ],
        out_specs=(
            pl.BlockSpec(memory_space=pltpu.VMEM),
            pl.BlockSpec(memory_space=pltpu.VMEM),
            pl.BlockSpec(memory_space=pltpu.VMEM),
        ),
        scratch_shapes=[
            pltpu.VMEM((size // 2, total // heads), jnp.float32),
            pltpu.VMEM((1, size), jnp.float32),
            pltpu.VMEM((total, size), raw_keys.dtype),
            pltpu.VMEM((total, size), jnp.float32),
            pltpu.VMEM((total, size), jnp.float32),
            pltpu.VMEM((total, size), jnp.float32),
            pltpu.SemaphoreType.DMA((len(set(even + odd)),)),
            pltpu.SemaphoreType.DMA((len(set(even + odd)),)),
            pltpu.SemaphoreType.REGULAR((devices,)),
            pltpu.SemaphoreType.DMA((4,)),
        ],
        compiler_params=pltpu.CompilerParams(
            collective_id=0, has_side_effects=True, vmem_limit_bytes=48 * 1024 * 1024
        ),
        name="exchange",
    )(raw_keys.reshape(flat), raw_values, turn_angle.T, key_gain.reshape(1, size))
    out = jax.ShapeDtypeStruct((total, size), raw_keys.dtype)
    in_vmem = pl.BlockSpec(memory_space=pltpu.VMEM)
    anywhere = pl.BlockSpec(memory_space=pl.ANY)
    keys, values, scale, after = pl.pallas_call(
        place_kernel,
        out_shape=(
            out, out, jax.ShapeDtypeStruct((heads, size), jnp.float32),
            jax.ShapeDtypeStruct((heads, size), jnp.float32),
        ),
        in_specs=[in_vmem] * 3,
        out_specs=[anywhere] * 4,
        scratch_shapes=[pltpu.SemaphoreType.DMA((3, WRITES))],
        compiler_params=pltpu.CompilerParams(vmem_limit_bytes=12 * 1024 * 1024),
        name="place",
    )(keys, values, scale)
    late = pl.pallas_call(
        functools.partial(tail_kernel, far_size, near_size),
        out_shape=pltpu.VMEM((sum(copy[2] for copy in tail), size), raw_keys.dtype),
        in_specs=[anywhere, anywhere],
        out_specs=in_vmem,
        scratch_shapes=[pltpu.SemaphoreType.DMA((len(tail),))] * 2,
        compiler_params=pltpu.CompilerParams(
            collective_id=1, has_side_effects=True, vmem_limit_bytes=TAIL_VMEM
        ),
        name="tail",
    )(raw_values, after)
    values = pl.pallas_call(
        functools.partial(place_tail_kernel, far_size, near_size, rows),
        out_shape=out,
        in_specs=[anywhere, in_vmem],
        out_specs=anywhere,
        input_output_aliases={0: 0},
        scratch_shapes=[pltpu.SemaphoreType.DMA((len(tail),))],
        compiler_params=pltpu.CompilerParams(vmem_limit_bytes=12 * 1024 * 1024),
        name="place_tail",
    )(values, late)
    full = (1, positions * devices, heads, size)
    return keys.reshape(full), values.reshape(full), scale.reshape(1, heads, size)


def solution(mesh):
    in_specs = (
        P(None, (FAR, NEAR), "model", None),
        P(None, (FAR, NEAR), "model", None),
        P(),
        P(),
    )
    out_specs = (
        P((FAR, NEAR), None, "model", None),
        P((FAR, NEAR), None, "model", None),
        P((FAR, NEAR), "model", None),
    )
    body = functools.partial(local, mesh.shape[FAR], mesh.shape[NEAR])
    return jax.shard_map(body, mesh=mesh, in_specs=in_specs, out_specs=out_specs, check_vma=False)
```

```python
import functools

import jax
import jax.numpy as jnp
from jax import lax
from jax.experimental import pallas as pl
from jax.experimental.pallas import tpu as pltpu
from jax.sharding import PartitionSpec as P

FAR, NEAR = "farcp", "nearcp"
MESH_ID = pl.DeviceIdType.MESH
TILE = 256
LATE = 15
HEAD = 2
LAST = 4
MOVED = 4
TAIL_VMEM = 51 * 1024 * 1024
WRITES = 4
LANES = 128


def step_kinds(far_size, near_size):
    kinds = {"both": [], "first": [], "second": [], "same": []}
    for step in range(1, far_size * near_size):
        far, chip = step // near_size > 0, step % near_size > 1
        kinds["both" if far and chip else "first" if far else "second" if chip else "same"].append(step)
    return kinds


def mixed(*lists):
    order = []
    for turn in range(max(map(len, lists))):
        order += [steps[turn] for steps in lists if turn < len(steps)]
    return order


def late_rows(rows):
    return rows * LATE // (16 * LANES) * LANES


def exchange_plan(far_size, near_size, rows):
    kinds = step_kinds(far_size, near_size)
    both, first, second, same = (kinds[kind] for kind in ("both", "first", "second", "same"))
    late = late_rows(rows)
    early = rows - late

    def straight(steps, parity):
        return [step for step in steps if step % 2 == parity]

    def whole(which, steps):
        copies = []
        for step in steps:
            head = HEAD * LANES if which == 0 and step == near_size else 0
            copies += [(which, step, 0, head)] if head else []
            copies.append((which, step, head, rows - head))
        return copies

    crossing = mixed(straight(first, 1), straight(second, 1), straight(both, 1)) + straight(same, 1)
    part = [(1, step, 0, early) for step in straight(both, 0)] if early else []
    rest = [(1, step, early, late) for step in straight(both, 0)]
    last, moved = LAST * LANES, MOVED * LANES
    even = whole(0, second + mixed(both, first) + same) + part
    even += [(1, step, 0, moved) for step in straight(second, 0)] + whole(1, crossing)
    odd = whole(0, second + mixed(first, both) + same) + whole(1, crossing) + part
    odd += whole(1, mixed(straight(first, 0), straight(second, 0))) + rest
    corner = mixed(
        [(step, 0, rows - last) for step in straight(first, 0)],
        [(step, moved, rows - moved) for step in straight(second, 0)],
    )
    corner += [(step, early, late) for step in straight(both, 0)]
    return even, odd, corner + [(step, rows - last, last) for step in straight(first, 0)]


def position(near_size):
    return lax.axis_index(FAR) * near_size + lax.axis_index(NEAR)


def device(index, near_size):
    return {FAR: index // near_size, NEAR: index % near_size}


def signal(semaphore, index, near_size):
    pl.semaphore_signal(
        semaphore, inc=1, device_id=device(index, near_size), device_id_type=MESH_ID
    )


def greet(barrier, me, near_size, steps):
    for step in steps:
        signal(barrier, me ^ step, near_size)
    pl.semaphore_wait(barrier, len(steps))


def greet_upwards(barrier, ready, me, near_size, steps):
    below = 0
    for step in steps:
        below += jnp.where((me & step) == step, 1, 0)
        pl.when((me & step) == 0)(functools.partial(signal, barrier, me ^ step, near_size))
    pl.when(me > 0)(functools.partial(pl.semaphore_wait, barrier, below))
    for step in steps:
        answer = functools.partial(signal, ready.at[step], me ^ step, near_size)
        pl.when((me & step) == step)(answer)


def exchange_kernel(
    far_size, near_size, heads, keys_ref, values_ref, turn_ref, plain_gain_ref,
    out_keys, out_values, out_scale,
    angle_ref, gain_ref, landed, cos_table, sin_table, turned, send_sem, recv_sem, ready, local_sem,
):
    me = position(near_size)
    rows = keys_ref.shape[1]
    total_rows = landed.shape[0]
    half = angle_ref.shape[0]
    devices = far_size * near_size
    even, odd, _ = exchange_plan(far_size, near_size, rows)
    slot = {copy: i for i, copy in enumerate(dict.fromkeys(even + odd))}

    angles = pltpu.make_async_copy(turn_ref, angle_ref, local_sem.at[2])
    gains = pltpu.make_async_copy(plain_gain_ref, gain_ref, local_sem.at[3])
    own = [
        pltpu.make_async_copy(src.at[me], dst.at[pl.ds(me * rows, rows)], local_sem.at[i])
        for i, (src, dst) in enumerate(((keys_ref, landed), (values_ref, out_values)))
    ]

    def remote(copy):
        which, step, offset, size = copy
        src, dst = ((keys_ref, landed), (values_ref, out_values))[which]
        return pltpu.make_async_remote_copy(
            src_ref=src.at[me ^ step, pl.ds(offset, size)],
            dst_ref=dst.at[pl.ds(me * rows + offset, size)],
            send_sem=send_sem.at[slot[copy]],
            recv_sem=recv_sem.at[slot[copy]],
            device_id=device(me ^ step, near_size),
            device_id_type=MESH_ID,
        )

    kinds = step_kinds(far_size, near_size)
    stages = (kinds["second"] + kinds["same"], kinds["first"], kinds["both"])
    greet_upwards(pltpu.get_barrier_semaphore(), ready, me, near_size, sum(stages, []))

    def wait_ready(steps):
        for step in steps:
            wait = functools.partial(pl.semaphore_wait, ready.at[step], 1)
            pl.when((me & step) == 0)(wait)

    head = (0, near_size, 0, HEAD * LANES)
    chip, turn = me // 2, near_size // 2
    before = chip == turn
    between = chip == 0

    pl.when(before)(remote(head).start)
    wait_ready(stages[0])
    for step in kinds["second"]:
        remote((0, step, 0, rows)).start()
    wait_ready(stages[1])
    pl.when(between)(remote(head).start)
    wait_ready(stages[2])
    for parity, copies in enumerate((even, odd)):

        @pl.when(me % 2 == parity)
        def _():
            for copy in copies[len(kinds["second"]) :]:
                if copy == head:
                    pl.when(~(before | between))(remote(copy).start)
                else:
                    remote(copy).start()

    for copy in (angles, gains, *own):
        copy.start()
    angles.wait()
    gains.wait()
    gain = gain_ref[...]
    other_gain = pltpu.roll(gain, half, 1)

    def fill(block, carry):
        angle = angle_ref[:, pl.ds(pl.multiple_of(block * LANES, LANES), LANES)]
        cosine, sine = jnp.cos(angle), jnp.sin(angle)
        cosine = jnp.concatenate([cosine, cosine], axis=0).T * gain
        sine = jnp.concatenate([-sine, sine], axis=0).T * other_gain
        for head in range(heads):
            place = pl.ds(block * (LANES * heads) + head, LANES, stride=heads)
            cos_table[place, :] = cosine
            sin_table[place, :] = sine
        return carry

    lax.fori_loop(0, total_rows // (heads * LANES), fill, 0)

    def prepare(owner, largest):
        def body(i, largest):
            place = pl.ds(pl.multiple_of(owner * rows + i * TILE, TILE), TILE)
            x = landed[place, :].astype(jnp.float32)
            mean = jnp.sum(x * x, axis=-1, keepdims=True) * (1.0 / x.shape[-1])
            x = x * lax.rsqrt(mean + 1e-06)
            t = x * cos_table[place, :] + pltpu.roll(x, half, 1) * sin_table[place, :]
            turned[place, :] = t
            return jnp.maximum(largest, jnp.max(jnp.abs(t).reshape(TILE // 8, 8, LANES), axis=0))

        return lax.fori_loop(0, rows // TILE, body, largest)

    largest = jnp.zeros((8, LANES), jnp.float32)
    own[0].wait()
    largest = prepare(me, largest)
    remote(head).wait_recv()
    for copy in even[devices - 1 :: -1]:
        if copy != head:
            remote(copy).wait_recv()
            largest = prepare(me ^ copy[1], largest)

    head_of = lax.broadcasted_iota(jnp.int32, (8, LANES), 0) % heads
    scale = jnp.zeros((8, LANES), jnp.float32)
    for head in range(heads):
        top = jnp.max(jnp.where(head_of == head, largest, 0.0), axis=0, keepdims=True)
        out_scale[pl.ds(head, 1), :] = top
        scale = jnp.where(head_of == head, top, scale)
    inverse = (1.0 / scale)[None]

    def narrow(i, carry):
        place = pl.ds(pl.multiple_of(i * TILE, TILE), TILE)
        t = turned[place, :].reshape(TILE // 8, 8, LANES) * inverse
        out_keys[place, :] = t.reshape(TILE, LANES).astype(out_keys.dtype)
        return carry

    lax.fori_loop(0, total_rows // TILE, narrow, 0)

    own[1].wait()
    for parity, mine, theirs in ((0, even, odd), (1, odd, even)):

        @pl.when(me % 2 == parity)
        def _():
            for copies, crossed in ((mine, 0), (theirs, 1)):
                for copy in copies:
                    if copy[0] == 1 and copy[1] % 2 == crossed:
                        remote(copy).wait_recv()
            for copy in mine:
                remote(copy).wait_send()


def tail_kernel(far_size, near_size, values_ref, after_ref, out_ref, send_sem, recv_sem):
    me = position(near_size)
    rows = values_ref.shape[1]
    plan = exchange_plan(far_size, near_size, rows)[2]

    @pl.when(me % 2 == 0)
    def _():
        greet(pltpu.get_barrier_semaphore(), me, near_size, sorted({step for step, _, _ in plan}))
        copies, place = {}, 0
        for i, (step, offset, size) in enumerate(plan):
            copies[step, offset] = (
                pltpu.make_async_remote_copy(
                    src_ref=values_ref.at[me ^ step, pl.ds(offset, size)],
                    dst_ref=out_ref.at[pl.ds(place, size)],
                    send_sem=send_sem.at[i],
                    recv_sem=recv_sem.at[i],
                    device_id=device(me ^ step, near_size),
                    device_id_type=MESH_ID,
                )
            )
            place += size
        kinds = step_kinds(far_size, near_size)
        inner = [copy for copy in plan if copy[0] not in kinds["both"]]
        outer = [copy for copy in plan if copy[0] in kinds["both"]]
        bent = me == near_size
        for order, here in ((inner + outer, bent), (plan, ~bent)):

            @pl.when(here)
            def _():
                for step, offset, _ in order:
                    copies[step, offset].start()

        for copy in copies.values():
            copy.wait_recv()
        for copy in copies.values():
            copy.wait_send()


def place_kernel(
    keys_ref, values_ref, scale_ref, out_keys, out_values, out_scale, after_ref, sem
):
    part = keys_ref.shape[0] // WRITES
    copies = [
        pltpu.make_async_copy(scale_ref, dst, sem.at[2, i]) for i, dst in enumerate((out_scale, after_ref))
    ]
    for i, (src, dst) in enumerate(((keys_ref, out_keys), (values_ref, out_values))):
        for j in range(WRITES):
            place = pl.ds(j * part, part)
            copies.append(pltpu.make_async_copy(src.at[place], dst.at[place], sem.at[i, j]))
    for copy in copies:
        copy.start()
    for copy in copies:
        copy.wait()


def place_tail_kernel(far_size, near_size, rows, values_ref, late_ref, out_ref, sem):
    me = position(near_size)

    @pl.when(me % 2 == 0)
    def _():
        copies, place = [], 0
        for i, (step, offset, size) in enumerate(exchange_plan(far_size, near_size, rows)[2]):
            copies.append(
                pltpu.make_async_copy(
                    late_ref.at[pl.ds(place, size)],
                    out_ref.at[pl.ds((me ^ step) * rows + offset, size)],
                    sem.at[i],
                )
            )
            place += size
        for copy in copies:
            copy.start()
        for copy in copies:
            copy.wait()


def local(far_size, near_size, raw_keys, raw_values, turn_angle, key_gain):
    sequences, positions, heads, size = raw_keys.shape
    devices = far_size * near_size
    rows = positions * heads
    total = rows * devices
    flat = (sequences, rows, size)
    even, odd, tail = exchange_plan(far_size, near_size, rows)
    raw_values = raw_values.reshape(flat)
    whole = pltpu.VMEM((total, size), raw_keys.dtype)
    keys, values, scale = pl.pallas_call(
        functools.partial(exchange_kernel, far_size, near_size, heads),
        out_shape=(whole, whole, pltpu.VMEM((heads, size), jnp.float32)),
        in_specs=[
            pl.BlockSpec(memory_space=pl.ANY),
            pl.BlockSpec(memory_space=pl.ANY),
            pl.BlockSpec(memory_space=pl.ANY),
            pl.BlockSpec(memory_space=pl.ANY),
        ],
        out_specs=(
            pl.BlockSpec(memory_space=pltpu.VMEM),
            pl.BlockSpec(memory_space=pltpu.VMEM),
            pl.BlockSpec(memory_space=pltpu.VMEM),
        ),
        scratch_shapes=[
            pltpu.VMEM((size // 2, total // heads), jnp.float32),
            pltpu.VMEM((1, size), jnp.float32),
            pltpu.VMEM((total, size), raw_keys.dtype),
            pltpu.VMEM((total, size), jnp.float32),
            pltpu.VMEM((total, size), jnp.float32),
            pltpu.VMEM((total, size), jnp.float32),
            pltpu.SemaphoreType.DMA((len(set(even + odd)),)),
            pltpu.SemaphoreType.DMA((len(set(even + odd)),)),
            pltpu.SemaphoreType.REGULAR((devices,)),
            pltpu.SemaphoreType.DMA((4,)),
        ],
        compiler_params=pltpu.CompilerParams(
            collective_id=0, has_side_effects=True, vmem_limit_bytes=48 * 1024 * 1024
        ),
        name="exchange",
    )(raw_keys.reshape(flat), raw_values, turn_angle.T, key_gain.reshape(1, size))
    out = jax.ShapeDtypeStruct((total, size), raw_keys.dtype)
    in_vmem = pl.BlockSpec(memory_space=pltpu.VMEM)
    anywhere = pl.BlockSpec(memory_space=pl.ANY)
    keys, values, scale, after = pl.pallas_call(
        place_kernel,
        out_shape=(
            out, out, jax.ShapeDtypeStruct((heads, size), jnp.float32),
            jax.ShapeDtypeStruct((heads, size), jnp.float32),
        ),
        in_specs=[in_vmem] * 3,
        out_specs=[anywhere] * 4,
        scratch_shapes=[pltpu.SemaphoreType.DMA((3, WRITES))],
        compiler_params=pltpu.CompilerParams(vmem_limit_bytes=12 * 1024 * 1024),
        name="place",
    )(keys, values, scale)
    late = pl.pallas_call(
        functools.partial(tail_kernel, far_size, near_size),
        out_shape=pltpu.VMEM((sum(copy[2] for copy in tail), size), raw_keys.dtype),
        in_specs=[anywhere, anywhere],
        out_specs=in_vmem,
        scratch_shapes=[pltpu.SemaphoreType.DMA((len(tail),))] * 2,
        compiler_params=pltpu.CompilerParams(
            collective_id=1, has_side_effects=True, vmem_limit_bytes=TAIL_VMEM
        ),
        name="tail",
    )(raw_values, after)
    values = pl.pallas_call(
        functools.partial(place_tail_kernel, far_size, near_size, rows),
        out_shape=out,
        in_specs=[anywhere, in_vmem],
        out_specs=anywhere,
        input_output_aliases={0: 0},
        scratch_shapes=[pltpu.SemaphoreType.DMA((len(tail),))],
        compiler_params=pltpu.CompilerParams(vmem_limit_bytes=12 * 1024 * 1024),
        name="place_tail",
    )(values, late)
    full = (1, positions * devices, heads, size)
    return keys.reshape(full), values.reshape(full), scale.reshape(1, heads, size)


def solution(mesh):
    in_specs = (
        P(None, (FAR, NEAR), "model", None),
        P(None, (FAR, NEAR), "model", None),
        P(),
        P(),
    )
    out_specs = (
        P((FAR, NEAR), None, "model", None),
        P((FAR, NEAR), None, "model", None),
        P((FAR, NEAR), "model", None),
    )
    body = functools.partial(local, mesh.shape[FAR], mesh.shape[NEAR])
    return jax.shard_map(body, mesh=mesh, in_specs=in_specs, out_specs=out_specs, check_vma=False)
```

```python
import functools

import jax
import jax.numpy as jnp
from jax import lax
from jax.experimental import pallas as pl
from jax.experimental.pallas import tpu as pltpu
from jax.sharding import PartitionSpec as P

FAR, NEAR = "farcp", "nearcp"
MESH_ID = pl.DeviceIdType.MESH
TILE = 256
LATE = 14
RELAY = 64
HEAD = 2
LAST = 4
MOVED = 4
TAIL_VMEM = 51 * 1024 * 1024
WRITES = 4
LANES = 128


def step_kinds(far_size, near_size):
    kinds = {"both": [], "first": [], "second": [], "same": []}
    for step in range(1, far_size * near_size):
        far, chip = step // near_size > 0, step % near_size > 1
        kinds["both" if far and chip else "first" if far else "second" if chip else "same"].append(step)
    return kinds


def mixed(*lists):
    order = []
    for turn in range(max(map(len, lists))):
        order += [steps[turn] for steps in lists if turn < len(steps)]
    return order


def late_rows(rows):
    return rows * LATE // (16 * LANES) * LANES


def relayed_copy(near_size):
    return (1, near_size + 2, 0, RELAY)


def exchange_plan(far_size, near_size, rows):
    kinds = step_kinds(far_size, near_size)
    both, first, second, same = (kinds[kind] for kind in ("both", "first", "second", "same"))
    late = late_rows(rows)
    early = rows - late

    def straight(steps, parity):
        return [step for step in steps if step % 2 == parity]

    def whole(which, steps):
        copies = []
        for step in steps:
            head = HEAD * LANES if which == 0 and step == near_size else 0
            copies += [(which, step, 0, head)] if head else []
            copies.append((which, step, head, rows - head))
        return copies

    crossing = mixed(straight(first, 1), straight(second, 1), straight(both, 1)) + straight(same, 1)
    part = [relayed_copy(near_size)]
    for step in straight(both, 0):
        skip = RELAY if step == part[0][1] else 0
        part.append((1, step, skip, early - skip))
    rest = [(1, step, early, late) for step in straight(both, 0)]
    last, moved = LAST * LANES, MOVED * LANES
    even = whole(0, second + mixed(both, first) + same) + part
    even += [(1, step, 0, moved) for step in straight(second, 0)] + whole(1, crossing)
    odd = whole(0, second + mixed(first, both) + same) + whole(1, crossing) + part
    odd += whole(1, mixed(straight(first, 0), straight(second, 0))) + rest
    corner = mixed(
        [(step, 0, rows - last) for step in straight(first, 0)],
        [(step, moved, rows - moved) for step in straight(second, 0)],
    )
    corner += [(step, early, late) for step in straight(both, 0)]
    return even, odd, corner + [(step, rows - last, last) for step in straight(first, 0)]


def position(near_size):
    return lax.axis_index(FAR) * near_size + lax.axis_index(NEAR)


def device(index, near_size):
    return {FAR: index // near_size, NEAR: index % near_size}


def signal(semaphore, index, near_size):
    pl.semaphore_signal(
        semaphore, inc=1, device_id=device(index, near_size), device_id_type=MESH_ID
    )


def greet(barrier, me, near_size, steps):
    for step in steps:
        signal(barrier, me ^ step, near_size)
    pl.semaphore_wait(barrier, len(steps))


def greet_upwards(barrier, ready, me, near_size, steps):
    below = 0
    for step in steps:
        below += jnp.where((me & step) == step, 1, 0)
        pl.when((me & step) == 0)(functools.partial(signal, barrier, me ^ step, near_size))
    pl.when(me > 0)(functools.partial(pl.semaphore_wait, barrier, below))
    for step in steps:
        answer = functools.partial(signal, ready.at[step], me ^ step, near_size)
        pl.when((me & step) == step)(answer)


def exchange_kernel(
    far_size, near_size, heads, keys_ref, values_ref, turn_ref, plain_gain_ref,
    out_keys, out_values, out_scale,
    angle_ref, gain_ref, landed, cos_table, sin_table, turned, held,
    send_sem, recv_sem, relay_sem, ready, local_sem,
):
    me = position(near_size)
    rows = keys_ref.shape[1]
    total_rows = landed.shape[0]
    half = angle_ref.shape[0]
    devices = far_size * near_size
    even, odd, _ = exchange_plan(far_size, near_size, rows)
    slot = {copy: i for i, copy in enumerate(dict.fromkeys(even + odd))}

    angles = pltpu.make_async_copy(turn_ref, angle_ref, local_sem.at[2])
    gains = pltpu.make_async_copy(plain_gain_ref, gain_ref, local_sem.at[3])
    own = [
        pltpu.make_async_copy(src.at[me], dst.at[pl.ds(me * rows, rows)], local_sem.at[i])
        for i, (src, dst) in enumerate(((keys_ref, landed), (values_ref, out_values)))
    ]

    def remote(copy):
        which, step, offset, size = copy
        src, dst = ((keys_ref, landed), (values_ref, out_values))[which]
        return pltpu.make_async_remote_copy(
            src_ref=src.at[me ^ step, pl.ds(offset, size)],
            dst_ref=dst.at[pl.ds(me * rows + offset, size)],
            send_sem=send_sem.at[slot[copy]],
            recv_sem=recv_sem.at[slot[copy]],
            device_id=device(me ^ step, near_size),
            device_id_type=MESH_ID,
        )

    kinds = step_kinds(far_size, near_size)
    stages = (kinds["second"] + kinds["same"], kinds["first"], kinds["both"])
    greet_upwards(pltpu.get_barrier_semaphore(), ready, me, near_size, sum(stages, []))

    def wait_ready(steps):
        for step in steps:
            wait = functools.partial(pl.semaphore_wait, ready.at[step], 1)
            pl.when((me & step) == 0)(wait)

    head = (0, near_size, 0, HEAD * LANES)
    chip, turn = me // 2, near_size // 2
    before = chip == turn
    between = chip == 0

    relayed = relayed_copy(near_size)
    to_relay = pltpu.make_async_remote_copy(
        src_ref=values_ref.at[me ^ relayed[1], pl.ds(0, RELAY)],
        dst_ref=held,
        send_sem=relay_sem.at[0],
        recv_sem=relay_sem.at[1],
        device_id=device(me ^ 2, near_size),
        device_id_type=MESH_ID,
    )
    from_relay = pltpu.make_async_remote_copy(
        src_ref=held,
        dst_ref=out_values.at[pl.ds((me ^ 2) * rows, RELAY)],
        send_sem=relay_sem.at[2],
        recv_sem=recv_sem.at[slot[relayed]],
        device_id=device(me ^ near_size, near_size),
        device_id_type=MESH_ID,
    )
    source, relay = chip == turn + 1, chip == turn

    pl.when(before)(remote(head).start)
    wait_ready(stages[0])
    pl.when(source)(to_relay.start)
    for step in kinds["second"]:
        remote((0, step, 0, rows)).start()
    wait_ready(stages[1])
    pl.when(between)(remote(head).start)
    wait_ready(stages[2])
    for parity, copies in enumerate((even, odd)):

        @pl.when(me % 2 == parity)
        def _():
            for copy in copies[len(kinds["second"]) :]:
                if copy == head:
                    pl.when(~(before | between))(remote(copy).start)
                elif copy == relayed:

                    @pl.when(relay)
                    def _():
                        to_relay.wait_recv()
                        from_relay.start()

                    pl.when(~source)(remote(copy).start)
                else:
                    remote(copy).start()

    for copy in (angles, gains, *own):
        copy.start()
    angles.wait()
    gains.wait()
    gain = gain_ref[...]
    other_gain = pltpu.roll(gain, half, 1)

    def fill(block, carry):
        angle = angle_ref[:, pl.ds(pl.multiple_of(block * LANES, LANES), LANES)]
        cosine, sine = jnp.cos(angle), jnp.sin(angle)
        cosine = jnp.concatenate([cosine, cosine], axis=0).T * gain
        sine = jnp.concatenate([-sine, sine], axis=0).T * other_gain
        for head in range(heads):
            place = pl.ds(block * (LANES * heads) + head, LANES, stride=heads)
            cos_table[place, :] = cosine
            sin_table[place, :] = sine
        return carry

    lax.fori_loop(0, total_rows // (heads * LANES), fill, 0)

    def prepare(owner, largest):
        def body(i, largest):
            place = pl.ds(pl.multiple_of(owner * rows + i * TILE, TILE), TILE)
            x = landed[place, :].astype(jnp.float32)
            mean = jnp.sum(x * x, axis=-1, keepdims=True) * (1.0 / x.shape[-1])
            x = x * lax.rsqrt(mean + 1e-06)
            t = x * cos_table[place, :] + pltpu.roll(x, half, 1) * sin_table[place, :]
            turned[place, :] = t
            return jnp.maximum(largest, jnp.max(jnp.abs(t).reshape(TILE // 8, 8, LANES), axis=0))

        return lax.fori_loop(0, rows // TILE, body, largest)

    largest = jnp.zeros((8, LANES), jnp.float32)
    own[0].wait()
    largest = prepare(me, largest)
    remote(head).wait_recv()
    for copy in even[devices - 1 :: -1]:
        if copy != head:
            remote(copy).wait_recv()
            largest = prepare(me ^ copy[1], largest)

    head_of = lax.broadcasted_iota(jnp.int32, (8, LANES), 0) % heads
    scale = jnp.zeros((8, LANES), jnp.float32)
    for head in range(heads):
        top = jnp.max(jnp.where(head_of == head, largest, 0.0), axis=0, keepdims=True)
        out_scale[pl.ds(head, 1), :] = top
        scale = jnp.where(head_of == head, top, scale)
    inverse = (1.0 / scale)[None]

    def narrow(i, carry):
        place = pl.ds(pl.multiple_of(i * TILE, TILE), TILE)
        t = turned[place, :].reshape(TILE // 8, 8, LANES) * inverse
        out_keys[place, :] = t.reshape(TILE, LANES).astype(out_keys.dtype)
        return carry

    lax.fori_loop(0, total_rows // TILE, narrow, 0)

    own[1].wait()
    for parity, mine, theirs in ((0, even, odd), (1, odd, even)):

        @pl.when(me % 2 == parity)
        def _():
            for copies, crossed in ((mine, 0), (theirs, 1)):
                for copy in copies:
                    if copy[0] == 1 and copy[1] % 2 == crossed:
                        remote(copy).wait_recv()
            for copy in mine:
                if copy == relayed:
                    pl.when(source)(to_relay.wait_send)
                    pl.when(relay)(from_relay.wait_send)
                    pl.when(~source)(remote(copy).wait_send)
                else:
                    remote(copy).wait_send()


def tail_kernel(far_size, near_size, values_ref, after_ref, out_ref, send_sem, recv_sem):
    me = position(near_size)
    rows = values_ref.shape[1]
    plan = exchange_plan(far_size, near_size, rows)[2]

    @pl.when(me % 2 == 0)
    def _():
        greet(pltpu.get_barrier_semaphore(), me, near_size, sorted({step for step, _, _ in plan}))
        copies, place = {}, 0
        for i, (step, offset, size) in enumerate(plan):
            copies[step, offset] = (
                pltpu.make_async_remote_copy(
                    src_ref=values_ref.at[me ^ step, pl.ds(offset, size)],
                    dst_ref=out_ref.at[pl.ds(place, size)],
                    send_sem=send_sem.at[i],
                    recv_sem=recv_sem.at[i],
                    device_id=device(me ^ step, near_size),
                    device_id_type=MESH_ID,
                )
            )
            place += size
        kinds = step_kinds(far_size, near_size)
        inner = [copy for copy in plan if copy[0] not in kinds["both"]]
        outer = [copy for copy in plan if copy[0] in kinds["both"]]
        bent = me == near_size
        for order, here in ((inner + outer, bent), (plan, ~bent)):

            @pl.when(here)
            def _():
                for step, offset, _ in order:
                    copies[step, offset].start()

        for copy in copies.values():
            copy.wait_recv()
        for copy in copies.values():
            copy.wait_send()


def place_kernel(
    keys_ref, values_ref, scale_ref, out_keys, out_values, out_scale, after_ref, sem
):
    part = keys_ref.shape[0] // WRITES
    copies = [
        pltpu.make_async_copy(scale_ref, dst, sem.at[2, i]) for i, dst in enumerate((out_scale, after_ref))
    ]
    for i, (src, dst) in enumerate(((keys_ref, out_keys), (values_ref, out_values))):
        for j in range(WRITES):
            place = pl.ds(j * part, part)
            copies.append(pltpu.make_async_copy(src.at[place], dst.at[place], sem.at[i, j]))
    for copy in copies:
        copy.start()
    for copy in copies:
        copy.wait()


def place_tail_kernel(far_size, near_size, rows, values_ref, late_ref, out_ref, sem):
    me = position(near_size)

    @pl.when(me % 2 == 0)
    def _():
        copies, place = [], 0
        for i, (step, offset, size) in enumerate(exchange_plan(far_size, near_size, rows)[2]):
            copies.append(
                pltpu.make_async_copy(
                    late_ref.at[pl.ds(place, size)],
                    out_ref.at[pl.ds((me ^ step) * rows + offset, size)],
                    sem.at[i],
                )
            )
            place += size
        for copy in copies:
            copy.start()
        for copy in copies:
            copy.wait()


def local(far_size, near_size, raw_keys, raw_values, turn_angle, key_gain):
    sequences, positions, heads, size = raw_keys.shape
    devices = far_size * near_size
    rows = positions * heads
    total = rows * devices
    flat = (sequences, rows, size)
    even, odd, tail = exchange_plan(far_size, near_size, rows)
    raw_values = raw_values.reshape(flat)
    whole = pltpu.VMEM((total, size), raw_keys.dtype)
    keys, values, scale = pl.pallas_call(
        functools.partial(exchange_kernel, far_size, near_size, heads),
        out_shape=(whole, whole, pltpu.VMEM((heads, size), jnp.float32)),
        in_specs=[
            pl.BlockSpec(memory_space=pl.ANY),
            pl.BlockSpec(memory_space=pl.ANY),
            pl.BlockSpec(memory_space=pl.ANY),
            pl.BlockSpec(memory_space=pl.ANY),
        ],
        out_specs=(
            pl.BlockSpec(memory_space=pltpu.VMEM),
            pl.BlockSpec(memory_space=pltpu.VMEM),
            pl.BlockSpec(memory_space=pltpu.VMEM),
        ),
        scratch_shapes=[
            pltpu.VMEM((size // 2, total // heads), jnp.float32),
            pltpu.VMEM((1, size), jnp.float32),
            pltpu.VMEM((total, size), raw_keys.dtype),
            pltpu.VMEM((total, size), jnp.float32),
            pltpu.VMEM((total, size), jnp.float32),
            pltpu.VMEM((total, size), jnp.float32),
            pltpu.VMEM((RELAY, size), raw_keys.dtype),
            pltpu.SemaphoreType.DMA((len(set(even + odd)),)),
            pltpu.SemaphoreType.DMA((len(set(even + odd)),)),
            pltpu.SemaphoreType.DMA((3,)),
            pltpu.SemaphoreType.REGULAR((devices,)),
            pltpu.SemaphoreType.DMA((4,)),
        ],
        compiler_params=pltpu.CompilerParams(
            collective_id=0, has_side_effects=True, vmem_limit_bytes=48 * 1024 * 1024
        ),
        name="exchange",
    )(raw_keys.reshape(flat), raw_values, turn_angle.T, key_gain.reshape(1, size))
    out = jax.ShapeDtypeStruct((total, size), raw_keys.dtype)
    in_vmem = pl.BlockSpec(memory_space=pltpu.VMEM)
    anywhere = pl.BlockSpec(memory_space=pl.ANY)
    keys, values, scale, after = pl.pallas_call(
        place_kernel,
        out_shape=(
            out, out, jax.ShapeDtypeStruct((heads, size), jnp.float32),
            jax.ShapeDtypeStruct((heads, size), jnp.float32),
        ),
        in_specs=[in_vmem] * 3,
        out_specs=[anywhere] * 4,
        scratch_shapes=[pltpu.SemaphoreType.DMA((3, WRITES))],
        compiler_params=pltpu.CompilerParams(vmem_limit_bytes=12 * 1024 * 1024),
        name="place",
    )(keys, values, scale)
    late = pl.pallas_call(
        functools.partial(tail_kernel, far_size, near_size),
        out_shape=pltpu.VMEM((sum(copy[2] for copy in tail), size), raw_keys.dtype),
        in_specs=[anywhere, anywhere],
        out_specs=in_vmem,
        scratch_shapes=[pltpu.SemaphoreType.DMA((len(tail),))] * 2,
        compiler_params=pltpu.CompilerParams(
            collective_id=1, has_side_effects=True, vmem_limit_bytes=TAIL_VMEM
        ),
        name="tail",
    )(raw_values, after)
    values = pl.pallas_call(
        functools.partial(place_tail_kernel, far_size, near_size, rows),
        out_shape=out,
        in_specs=[anywhere, in_vmem],
        out_specs=anywhere,
        input_output_aliases={0: 0},
        scratch_shapes=[pltpu.SemaphoreType.DMA((len(tail),))],
        compiler_params=pltpu.CompilerParams(vmem_limit_bytes=12 * 1024 * 1024),
        name="place_tail",
    )(values, late)
    full = (1, positions * devices, heads, size)
    return keys.reshape(full), values.reshape(full), scale.reshape(1, heads, size)


def solution(mesh):
    in_specs = (
        P(None, (FAR, NEAR), "model", None),
        P(None, (FAR, NEAR), "model", None),
        P(),
        P(),
    )
    out_specs = (
        P((FAR, NEAR), None, "model", None),
        P((FAR, NEAR), None, "model", None),
        P((FAR, NEAR), "model", None),
    )
    body = functools.partial(local, mesh.shape[FAR], mesh.shape[NEAR])
    return jax.shard_map(body, mesh=mesh, in_specs=in_specs, out_specs=out_specs, check_vma=False)
```

```python
import functools

import jax
import jax.numpy as jnp
from jax import lax
from jax.experimental import pallas as pl
from jax.experimental.pallas import tpu as pltpu
from jax.sharding import PartitionSpec as P

FAR, NEAR = "farcp", "nearcp"
MESH_ID = pl.DeviceIdType.MESH
TILE = 256
LATE = 14
RELAY = 64
HEAD = 2
LAST = 3
MOVED = 3
TAIL_VMEM = 51 * 1024 * 1024
WRITES = 4
LANES = 128


def step_kinds(far_size, near_size):
    kinds = {"both": [], "first": [], "second": [], "same": []}
    for step in range(1, far_size * near_size):
        far, chip = step // near_size > 0, step % near_size > 1
        kinds["both" if far and chip else "first" if far else "second" if chip else "same"].append(step)
    return kinds


def mixed(*lists):
    order = []
    for turn in range(max(map(len, lists))):
        order += [steps[turn] for steps in lists if turn < len(steps)]
    return order


def late_rows(rows):
    return rows * LATE // (16 * LANES) * LANES


def relayed_copy(near_size):
    return (1, near_size + 2, 0, RELAY)


def exchange_plan(far_size, near_size, rows):
    kinds = step_kinds(far_size, near_size)
    both, first, second, same = (kinds[kind] for kind in ("both", "first", "second", "same"))
    late = late_rows(rows)
    early = rows - late

    def straight(steps, parity):
        return [step for step in steps if step % 2 == parity]

    def whole(which, steps):
        copies = []
        for step in steps:
            head = HEAD * LANES if which == 0 and step == near_size else 0
            copies += [(which, step, 0, head)] if head else []
            copies.append((which, step, head, rows - head))
        return copies

    crossing = mixed(straight(first, 1), straight(second, 1), straight(both, 1)) + straight(same, 1)
    part = [relayed_copy(near_size)]
    for step in straight(both, 0):
        skip = RELAY if step == part[0][1] else 0
        part.append((1, step, skip, early - skip))
    rest = [(1, step, early, late) for step in straight(both, 0)]
    last, moved = LAST * LANES, MOVED * LANES
    even = whole(0, second + mixed(both, first) + same) + part
    even += [(1, step, 0, moved) for step in straight(second, 0)] + whole(1, crossing)
    odd = whole(0, second + mixed(first, both) + same) + whole(1, crossing) + part
    odd += whole(1, mixed(straight(first, 0), straight(second, 0))) + rest
    corner = mixed(
        [(step, 0, rows - last) for step in straight(first, 0)],
        [(step, moved, rows - moved) for step in straight(second, 0)],
    )
    corner += [(step, early, late) for step in straight(both, 0)]
    return even, odd, corner + [(step, rows - last, last) for step in straight(first, 0)]


def position(near_size):
    return lax.axis_index(FAR) * near_size + lax.axis_index(NEAR)


def device(index, near_size):
    return {FAR: index // near_size, NEAR: index % near_size}


def signal(semaphore, index, near_size):
    pl.semaphore_signal(
        semaphore, inc=1, device_id=device(index, near_size), device_id_type=MESH_ID
    )


def greet(barrier, me, near_size, steps):
    for step in steps:
        signal(barrier, me ^ step, near_size)
    pl.semaphore_wait(barrier, len(steps))


def greet_upwards(barrier, ready, me, near_size, steps):
    below = 0
    for step in steps:
        below += jnp.where((me & step) == step, 1, 0)
        pl.when((me & step) == 0)(functools.partial(signal, barrier, me ^ step, near_size))
    pl.when(me > 0)(functools.partial(pl.semaphore_wait, barrier, below))
    for step in steps:
        answer = functools.partial(signal, ready.at[step], me ^ step, near_size)
        pl.when((me & step) == step)(answer)


def exchange_kernel(
    far_size, near_size, heads, keys_ref, values_ref, turn_ref, plain_gain_ref,
    out_keys, out_values, out_scale,
    angle_ref, gain_ref, landed, cos_table, sin_table, turned, held,
    send_sem, recv_sem, relay_sem, ready, local_sem,
):
    me = position(near_size)
    rows = keys_ref.shape[1]
    total_rows = landed.shape[0]
    half = angle_ref.shape[0]
    devices = far_size * near_size
    even, odd, _ = exchange_plan(far_size, near_size, rows)
    slot = {copy: i for i, copy in enumerate(dict.fromkeys(even + odd))}

    angles = pltpu.make_async_copy(turn_ref, angle_ref, local_sem.at[2])
    gains = pltpu.make_async_copy(plain_gain_ref, gain_ref, local_sem.at[3])
    own = [
        pltpu.make_async_copy(src.at[me], dst.at[pl.ds(me * rows, rows)], local_sem.at[i])
        for i, (src, dst) in enumerate(((keys_ref, landed), (values_ref, out_values)))
    ]

    def remote(copy):
        which, step, offset, size = copy
        src, dst = ((keys_ref, landed), (values_ref, out_values))[which]
        return pltpu.make_async_remote_copy(
            src_ref=src.at[me ^ step, pl.ds(offset, size)],
            dst_ref=dst.at[pl.ds(me * rows + offset, size)],
            send_sem=send_sem.at[slot[copy]],
            recv_sem=recv_sem.at[slot[copy]],
            device_id=device(me ^ step, near_size),
            device_id_type=MESH_ID,
        )

    kinds = step_kinds(far_size, near_size)
    stages = (kinds["second"] + kinds["same"], kinds["first"], kinds["both"])
    greet_upwards(pltpu.get_barrier_semaphore(), ready, me, near_size, sum(stages, []))

    def wait_ready(steps):
        for step in steps:
            wait = functools.partial(pl.semaphore_wait, ready.at[step], 1)
            pl.when((me & step) == 0)(wait)

    head = (0, near_size, 0, HEAD * LANES)
    chip, turn = me // 2, near_size // 2
    before = chip == turn
    between = chip == 0

    relayed = relayed_copy(near_size)
    to_relay = pltpu.make_async_remote_copy(
        src_ref=values_ref.at[me ^ relayed[1], pl.ds(0, RELAY)],
        dst_ref=held,
        send_sem=relay_sem.at[0],
        recv_sem=relay_sem.at[1],
        device_id=device(me ^ 2, near_size),
        device_id_type=MESH_ID,
    )
    from_relay = pltpu.make_async_remote_copy(
        src_ref=held,
        dst_ref=out_values.at[pl.ds((me ^ 2) * rows, RELAY)],
        send_sem=relay_sem.at[2],
        recv_sem=recv_sem.at[slot[relayed]],
        device_id=device(me ^ near_size, near_size),
        device_id_type=MESH_ID,
    )
    source, relay = chip == turn + 1, chip == turn

    pl.when(before)(remote(head).start)
    wait_ready(stages[0])
    pl.when(source)(to_relay.start)
    for step in kinds["second"]:
        remote((0, step, 0, rows)).start()
    wait_ready(stages[1])
    pl.when(between)(remote(head).start)
    wait_ready(stages[2])
    for parity, copies in enumerate((even, odd)):

        @pl.when(me % 2 == parity)
        def _():
            for copy in copies[len(kinds["second"]) :]:
                if copy == head:
                    pl.when(~(before | between))(remote(copy).start)
                elif copy == relayed:

                    @pl.when(relay)
                    def _():
                        to_relay.wait_recv()
                        from_relay.start()

                    pl.when(~source)(remote(copy).start)
                else:
                    remote(copy).start()

    for copy in (angles, gains, *own):
        copy.start()
    angles.wait()
    gains.wait()
    gain = gain_ref[...]
    other_gain = pltpu.roll(gain, half, 1)

    def fill(block, carry):
        angle = angle_ref[:, pl.ds(pl.multiple_of(block * LANES, LANES), LANES)]
        cosine, sine = jnp.cos(angle), jnp.sin(angle)
        cosine = jnp.concatenate([cosine, cosine], axis=0).T * gain
        sine = jnp.concatenate([-sine, sine], axis=0).T * other_gain
        for head in range(heads):
            place = pl.ds(block * (LANES * heads) + head, LANES, stride=heads)
            cos_table[place, :] = cosine
            sin_table[place, :] = sine
        return carry

    lax.fori_loop(0, total_rows // (heads * LANES), fill, 0)

    def prepare(owner, largest):
        def body(i, largest):
            place = pl.ds(pl.multiple_of(owner * rows + i * TILE, TILE), TILE)
            x = landed[place, :].astype(jnp.float32)
            mean = jnp.sum(x * x, axis=-1, keepdims=True) * (1.0 / x.shape[-1])
            x = x * lax.rsqrt(mean + 1e-06)
            t = x * cos_table[place, :] + pltpu.roll(x, half, 1) * sin_table[place, :]
            turned[place, :] = t
            return jnp.maximum(largest, jnp.max(jnp.abs(t).reshape(TILE // 8, 8, LANES), axis=0))

        return lax.fori_loop(0, rows // TILE, body, largest)

    largest = jnp.zeros((8, LANES), jnp.float32)
    own[0].wait()
    largest = prepare(me, largest)
    remote(head).wait_recv()
    for copy in even[devices - 1 :: -1]:
        if copy != head:
            remote(copy).wait_recv()
            largest = prepare(me ^ copy[1], largest)

    head_of = lax.broadcasted_iota(jnp.int32, (8, LANES), 0) % heads
    scale = jnp.zeros((8, LANES), jnp.float32)
    for head in range(heads):
        top = jnp.max(jnp.where(head_of == head, largest, 0.0), axis=0, keepdims=True)
        out_scale[pl.ds(head, 1), :] = top
        scale = jnp.where(head_of == head, top, scale)
    inverse = (1.0 / scale)[None]

    def narrow(i, carry):
        place = pl.ds(pl.multiple_of(i * TILE, TILE), TILE)
        t = turned[place, :].reshape(TILE // 8, 8, LANES) * inverse
        out_keys[place, :] = t.reshape(TILE, LANES).astype(out_keys.dtype)
        return carry

    lax.fori_loop(0, total_rows // TILE, narrow, 0)

    own[1].wait()
    for parity, mine, theirs in ((0, even, odd), (1, odd, even)):

        @pl.when(me % 2 == parity)
        def _():
            for copies, crossed in ((mine, 0), (theirs, 1)):
                for copy in copies:
                    if copy[0] == 1 and copy[1] % 2 == crossed:
                        remote(copy).wait_recv()
            for copy in mine:
                if copy == relayed:
                    pl.when(source)(to_relay.wait_send)
                    pl.when(relay)(from_relay.wait_send)
                    pl.when(~source)(remote(copy).wait_send)
                else:
                    remote(copy).wait_send()


def tail_kernel(far_size, near_size, values_ref, after_ref, out_ref, send_sem, recv_sem):
    me = position(near_size)
    rows = values_ref.shape[1]
    plan = exchange_plan(far_size, near_size, rows)[2]

    @pl.when(me % 2 == 0)
    def _():
        greet(pltpu.get_barrier_semaphore(), me, near_size, sorted({step for step, _, _ in plan}))
        copies, place = {}, 0
        for i, (step, offset, size) in enumerate(plan):
            copies[step, offset] = (
                pltpu.make_async_remote_copy(
                    src_ref=values_ref.at[me ^ step, pl.ds(offset, size)],
                    dst_ref=out_ref.at[pl.ds(place, size)],
                    send_sem=send_sem.at[i],
                    recv_sem=recv_sem.at[i],
                    device_id=device(me ^ step, near_size),
                    device_id_type=MESH_ID,
                )
            )
            place += size
        kinds = step_kinds(far_size, near_size)
        inner = [copy for copy in plan if copy[0] not in kinds["both"]]
        outer = [copy for copy in plan if copy[0] in kinds["both"]]
        bent = me == near_size
        for order, here in ((inner + outer, bent), (plan, ~bent)):

            @pl.when(here)
            def _():
                for step, offset, _ in order:
                    copies[step, offset].start()

        for copy in copies.values():
            copy.wait_recv()
        for copy in copies.values():
            copy.wait_send()


def place_kernel(
    keys_ref, values_ref, scale_ref, out_keys, out_values, out_scale, after_ref, sem
):
    part = keys_ref.shape[0] // WRITES
    copies = [
        pltpu.make_async_copy(scale_ref, dst, sem.at[2, i]) for i, dst in enumerate((out_scale, after_ref))
    ]
    for i, (src, dst) in enumerate(((keys_ref, out_keys), (values_ref, out_values))):
        for j in range(WRITES):
            place = pl.ds(j * part, part)
            copies.append(pltpu.make_async_copy(src.at[place], dst.at[place], sem.at[i, j]))
    for copy in copies:
        copy.start()
    for copy in copies:
        copy.wait()


def place_tail_kernel(far_size, near_size, rows, values_ref, late_ref, out_ref, sem):
    me = position(near_size)

    @pl.when(me % 2 == 0)
    def _():
        copies, place = [], 0
        for i, (step, offset, size) in enumerate(exchange_plan(far_size, near_size, rows)[2]):
            copies.append(
                pltpu.make_async_copy(
                    late_ref.at[pl.ds(place, size)],
                    out_ref.at[pl.ds((me ^ step) * rows + offset, size)],
                    sem.at[i],
                )
            )
            place += size
        for copy in copies:
            copy.start()
        for copy in copies:
            copy.wait()


def local(far_size, near_size, raw_keys, raw_values, turn_angle, key_gain):
    sequences, positions, heads, size = raw_keys.shape
    devices = far_size * near_size
    rows = positions * heads
    total = rows * devices
    flat = (sequences, rows, size)
    even, odd, tail = exchange_plan(far_size, near_size, rows)
    raw_values = raw_values.reshape(flat)
    whole = pltpu.VMEM((total, size), raw_keys.dtype)
    keys, values, scale = pl.pallas_call(
        functools.partial(exchange_kernel, far_size, near_size, heads),
        out_shape=(whole, whole, pltpu.VMEM((heads, size), jnp.float32)),
        in_specs=[
            pl.BlockSpec(memory_space=pl.ANY),
            pl.BlockSpec(memory_space=pl.ANY),
            pl.BlockSpec(memory_space=pl.ANY),
            pl.BlockSpec(memory_space=pl.ANY),
        ],
        out_specs=(
            pl.BlockSpec(memory_space=pltpu.VMEM),
            pl.BlockSpec(memory_space=pltpu.VMEM),
            pl.BlockSpec(memory_space=pltpu.VMEM),
        ),
        scratch_shapes=[
            pltpu.VMEM((size // 2, total // heads), jnp.float32),
            pltpu.VMEM((1, size), jnp.float32),
            pltpu.VMEM((total, size), raw_keys.dtype),
            pltpu.VMEM((total, size), jnp.float32),
            pltpu.VMEM((total, size), jnp.float32),
            pltpu.VMEM((total, size), jnp.float32),
            pltpu.VMEM((RELAY, size), raw_keys.dtype),
            pltpu.SemaphoreType.DMA((len(set(even + odd)),)),
            pltpu.SemaphoreType.DMA((len(set(even + odd)),)),
            pltpu.SemaphoreType.DMA((3,)),
            pltpu.SemaphoreType.REGULAR((devices,)),
            pltpu.SemaphoreType.DMA((4,)),
        ],
        compiler_params=pltpu.CompilerParams(
            collective_id=0, has_side_effects=True, vmem_limit_bytes=48 * 1024 * 1024
        ),
        name="exchange",
    )(raw_keys.reshape(flat), raw_values, turn_angle.T, key_gain.reshape(1, size))
    out = jax.ShapeDtypeStruct((total, size), raw_keys.dtype)
    in_vmem = pl.BlockSpec(memory_space=pltpu.VMEM)
    anywhere = pl.BlockSpec(memory_space=pl.ANY)
    keys, values, scale, after = pl.pallas_call(
        place_kernel,
        out_shape=(
            out, out, jax.ShapeDtypeStruct((heads, size), jnp.float32),
            jax.ShapeDtypeStruct((heads, size), jnp.float32),
        ),
        in_specs=[in_vmem] * 3,
        out_specs=[anywhere] * 4,
        scratch_shapes=[pltpu.SemaphoreType.DMA((3, WRITES))],
        compiler_params=pltpu.CompilerParams(vmem_limit_bytes=12 * 1024 * 1024),
        name="place",
    )(keys, values, scale)
    late = pl.pallas_call(
        functools.partial(tail_kernel, far_size, near_size),
        out_shape=pltpu.VMEM((sum(copy[2] for copy in tail), size), raw_keys.dtype),
        in_specs=[anywhere, anywhere],
        out_specs=in_vmem,
        scratch_shapes=[pltpu.SemaphoreType.DMA((len(tail),))] * 2,
        compiler_params=pltpu.CompilerParams(
            collective_id=1, has_side_effects=True, vmem_limit_bytes=TAIL_VMEM
        ),
        name="tail",
    )(raw_values, after)
    values = pl.pallas_call(
        functools.partial(place_tail_kernel, far_size, near_size, rows),
        out_shape=out,
        in_specs=[anywhere, in_vmem],
        out_specs=anywhere,
        input_output_aliases={0: 0},
        scratch_shapes=[pltpu.SemaphoreType.DMA((len(tail),))],
        compiler_params=pltpu.CompilerParams(vmem_limit_bytes=12 * 1024 * 1024),
        name="place_tail",
    )(values, late)
    full = (1, positions * devices, heads, size)
    return keys.reshape(full), values.reshape(full), scale.reshape(1, heads, size)


def solution(mesh):
    in_specs = (
        P(None, (FAR, NEAR), "model", None),
        P(None, (FAR, NEAR), "model", None),
        P(),
        P(),
    )
    out_specs = (
        P((FAR, NEAR), None, "model", None),
        P((FAR, NEAR), None, "model", None),
        P((FAR, NEAR), "model", None),
    )
    body = functools.partial(local, mesh.shape[FAR], mesh.shape[NEAR])
    return jax.shard_map(body, mesh=mesh, in_specs=in_specs, out_specs=out_specs, check_vma=False)
```

```python
import functools

import jax
import jax.numpy as jnp
from jax import lax
from jax.experimental import pallas as pl
from jax.experimental.pallas import tpu as pltpu
from jax.sharding import PartitionSpec as P

FAR, NEAR = "farcp", "nearcp"
MESH_ID = pl.DeviceIdType.MESH
TILE = 256
LATE = 14
RELAY = 64
HEAD = 3
LAST = 4
MOVED = 4
TAIL_VMEM = 51 * 1024 * 1024
WRITES = 4
LANES = 128


def step_kinds(far_size, near_size):
    kinds = {"both": [], "first": [], "second": [], "same": []}
    for step in range(1, far_size * near_size):
        far, chip = step // near_size > 0, step % near_size > 1
        kinds["both" if far and chip else "first" if far else "second" if chip else "same"].append(step)
    return kinds


def mixed(*lists):
    order = []
    for turn in range(max(map(len, lists))):
        order += [steps[turn] for steps in lists if turn < len(steps)]
    return order


def late_rows(rows):
    return rows * LATE // (16 * LANES) * LANES


def relayed_copy(near_size):
    return (1, near_size + 2, 0, RELAY)


def exchange_plan(far_size, near_size, rows):
    kinds = step_kinds(far_size, near_size)
    both, first, second, same = (kinds[kind] for kind in ("both", "first", "second", "same"))
    late = late_rows(rows)
    early = rows - late

    def straight(steps, parity):
        return [step for step in steps if step % 2 == parity]

    def whole(which, steps):
        copies = []
        for step in steps:
            head = HEAD * LANES if which == 0 and step == near_size else 0
            copies += [(which, step, 0, head)] if head else []
            copies.append((which, step, head, rows - head))
        return copies

    crossing = mixed(straight(first, 1), straight(second, 1), straight(both, 1)) + straight(same, 1)
    part = [relayed_copy(near_size)]
    for step in straight(both, 0):
        skip = RELAY if step == part[0][1] else 0
        part.append((1, step, skip, early - skip))
    rest = [(1, step, early, late) for step in straight(both, 0)]
    last, moved = LAST * LANES, MOVED * LANES
    even = whole(0, second + mixed(both, first) + same) + part
    even += [(1, step, 0, moved) for step in straight(second, 0)] + whole(1, crossing)
    odd = whole(0, second + mixed(first, both) + same) + whole(1, crossing) + part
    odd += whole(1, mixed(straight(first, 0), straight(second, 0))) + rest
    corner = mixed(
        [(step, 0, rows - last) for step in straight(first, 0)],
        [(step, moved, rows - moved) for step in straight(second, 0)],
    )
    corner += [(step, early, late) for step in straight(both, 0)]
    return even, odd, corner + [(step, rows - last, last) for step in straight(first, 0)]


def position(near_size):
    return lax.axis_index(FAR) * near_size + lax.axis_index(NEAR)


def device(index, near_size):
    return {FAR: index // near_size, NEAR: index % near_size}


def signal(semaphore, index, near_size):
    pl.semaphore_signal(
        semaphore, inc=1, device_id=device(index, near_size), device_id_type=MESH_ID
    )


def greet(barrier, me, near_size, steps):
    for step in steps:
        signal(barrier, me ^ step, near_size)
    pl.semaphore_wait(barrier, len(steps))


def greet_upwards(barrier, ready, me, near_size, steps):
    below = 0
    for step in steps:
        below += jnp.where((me & step) == step, 1, 0)
        pl.when((me & step) == 0)(functools.partial(signal, barrier, me ^ step, near_size))
    pl.when(me > 0)(functools.partial(pl.semaphore_wait, barrier, below))
    for step in steps:
        answer = functools.partial(signal, ready.at[step], me ^ step, near_size)
        pl.when((me & step) == step)(answer)


def exchange_kernel(
    far_size, near_size, heads, keys_ref, values_ref, turn_ref, plain_gain_ref,
    out_keys, out_values, out_scale,
    angle_ref, gain_ref, landed, cos_table, sin_table, turned, held,
    send_sem, recv_sem, relay_sem, ready, local_sem,
):
    me = position(near_size)
    rows = keys_ref.shape[1]
    total_rows = landed.shape[0]
    half = angle_ref.shape[0]
    devices = far_size * near_size
    even, odd, _ = exchange_plan(far_size, near_size, rows)
    slot = {copy: i for i, copy in enumerate(dict.fromkeys(even + odd))}

    angles = pltpu.make_async_copy(turn_ref, angle_ref, local_sem.at[2])
    gains = pltpu.make_async_copy(plain_gain_ref, gain_ref, local_sem.at[3])
    own = [
        pltpu.make_async_copy(src.at[me], dst.at[pl.ds(me * rows, rows)], local_sem.at[i])
        for i, (src, dst) in enumerate(((keys_ref, landed), (values_ref, out_values)))
    ]

    def remote(copy):
        which, step, offset, size = copy
        src, dst = ((keys_ref, landed), (values_ref, out_values))[which]
        return pltpu.make_async_remote_copy(
            src_ref=src.at[me ^ step, pl.ds(offset, size)],
            dst_ref=dst.at[pl.ds(me * rows + offset, size)],
            send_sem=send_sem.at[slot[copy]],
            recv_sem=recv_sem.at[slot[copy]],
            device_id=device(me ^ step, near_size),
            device_id_type=MESH_ID,
        )

    kinds = step_kinds(far_size, near_size)
    stages = (kinds["second"] + kinds["same"], kinds["first"], kinds["both"])
    greet_upwards(pltpu.get_barrier_semaphore(), ready, me, near_size, sum(stages, []))

    def wait_ready(steps):
        for step in steps:
            wait = functools.partial(pl.semaphore_wait, ready.at[step], 1)
            pl.when((me & step) == 0)(wait)

    head = (0, near_size, 0, HEAD * LANES)
    chip, turn = me // 2, near_size // 2
    before = chip == turn
    between = chip == 0

    relayed = relayed_copy(near_size)
    to_relay = pltpu.make_async_remote_copy(
        src_ref=values_ref.at[me ^ relayed[1], pl.ds(0, RELAY)],
        dst_ref=held,
        send_sem=relay_sem.at[0],
        recv_sem=relay_sem.at[1],
        device_id=device(me ^ 2, near_size),
        device_id_type=MESH_ID,
    )
    from_relay = pltpu.make_async_remote_copy(
        src_ref=held,
        dst_ref=out_values.at[pl.ds((me ^ 2) * rows, RELAY)],
        send_sem=relay_sem.at[2],
        recv_sem=recv_sem.at[slot[relayed]],
        device_id=device(me ^ near_size, near_size),
        device_id_type=MESH_ID,
    )
    source, relay = chip == turn + 1, chip == turn

    pl.when(before)(remote(head).start)
    wait_ready(stages[0])
    pl.when(source)(to_relay.start)
    for step in kinds["second"]:
        remote((0, step, 0, rows)).start()
    wait_ready(stages[1])
    pl.when(between)(remote(head).start)
    wait_ready(stages[2])
    for parity, copies in enumerate((even, odd)):

        @pl.when(me % 2 == parity)
        def _():
            for copy in copies[len(kinds["second"]) :]:
                if copy == head:
                    pl.when(~(before | between))(remote(copy).start)
                elif copy == relayed:

                    @pl.when(relay)
                    def _():
                        to_relay.wait_recv()
                        from_relay.start()

                    pl.when(~source)(remote(copy).start)
                else:
                    remote(copy).start()

    for copy in (angles, gains, *own):
        copy.start()
    angles.wait()
    gains.wait()
    gain = gain_ref[...]
    other_gain = pltpu.roll(gain, half, 1)

    def fill(block, carry):
        angle = angle_ref[:, pl.ds(pl.multiple_of(block * LANES, LANES), LANES)]
        cosine, sine = jnp.cos(angle), jnp.sin(angle)
        cosine = jnp.concatenate([cosine, cosine], axis=0).T * gain
        sine = jnp.concatenate([-sine, sine], axis=0).T * other_gain
        for head in range(heads):
            place = pl.ds(block * (LANES * heads) + head, LANES, stride=heads)
            cos_table[place, :] = cosine
            sin_table[place, :] = sine
        return carry

    lax.fori_loop(0, total_rows // (heads * LANES), fill, 0)

    def prepare(owner, largest):
        def body(i, largest):
            place = pl.ds(pl.multiple_of(owner * rows + i * TILE, TILE), TILE)
            x = landed[place, :].astype(jnp.float32)
            mean = jnp.sum(x * x, axis=-1, keepdims=True) * (1.0 / x.shape[-1])
            x = x * lax.rsqrt(mean + 1e-06)
            t = x * cos_table[place, :] + pltpu.roll(x, half, 1) * sin_table[place, :]
            turned[place, :] = t
            return jnp.maximum(largest, jnp.max(jnp.abs(t).reshape(TILE // 8, 8, LANES), axis=0))

        return lax.fori_loop(0, rows // TILE, body, largest)

    largest = jnp.zeros((8, LANES), jnp.float32)
    own[0].wait()
    largest = prepare(me, largest)
    remote(head).wait_recv()
    for copy in even[devices - 1 :: -1]:
        if copy != head:
            remote(copy).wait_recv()
            largest = prepare(me ^ copy[1], largest)

    head_of = lax.broadcasted_iota(jnp.int32, (8, LANES), 0) % heads
    scale = jnp.zeros((8, LANES), jnp.float32)
    for head in range(heads):
        top = jnp.max(jnp.where(head_of == head, largest, 0.0), axis=0, keepdims=True)
        out_scale[pl.ds(head, 1), :] = top
        scale = jnp.where(head_of == head, top, scale)
    inverse = (1.0 / scale)[None]

    def narrow(i, carry):
        place = pl.ds(pl.multiple_of(i * TILE, TILE), TILE)
        t = turned[place, :].reshape(TILE // 8, 8, LANES) * inverse
        out_keys[place, :] = t.reshape(TILE, LANES).astype(out_keys.dtype)
        return carry

    lax.fori_loop(0, total_rows // TILE, narrow, 0)

    own[1].wait()
    for parity, mine, theirs in ((0, even, odd), (1, odd, even)):

        @pl.when(me % 2 == parity)
        def _():
            for copies, crossed in ((mine, 0), (theirs, 1)):
                for copy in copies:
                    if copy[0] == 1 and copy[1] % 2 == crossed:
                        remote(copy).wait_recv()
            for copy in mine:
                if copy == relayed:
                    pl.when(source)(to_relay.wait_send)
                    pl.when(relay)(from_relay.wait_send)
                    pl.when(~source)(remote(copy).wait_send)
                else:
                    remote(copy).wait_send()


def tail_kernel(far_size, near_size, values_ref, after_ref, out_ref, send_sem, recv_sem):
    me = position(near_size)
    rows = values_ref.shape[1]
    plan = exchange_plan(far_size, near_size, rows)[2]

    @pl.when(me % 2 == 0)
    def _():
        greet(pltpu.get_barrier_semaphore(), me, near_size, sorted({step for step, _, _ in plan}))
        copies, place = {}, 0
        for i, (step, offset, size) in enumerate(plan):
            copies[step, offset] = (
                pltpu.make_async_remote_copy(
                    src_ref=values_ref.at[me ^ step, pl.ds(offset, size)],
                    dst_ref=out_ref.at[pl.ds(place, size)],
                    send_sem=send_sem.at[i],
                    recv_sem=recv_sem.at[i],
                    device_id=device(me ^ step, near_size),
                    device_id_type=MESH_ID,
                )
            )
            place += size
        kinds = step_kinds(far_size, near_size)
        inner = [copy for copy in plan if copy[0] not in kinds["both"]]
        outer = [copy for copy in plan if copy[0] in kinds["both"]]
        bent = me == near_size
        for order, here in ((inner + outer, bent), (plan, ~bent)):

            @pl.when(here)
            def _():
                for step, offset, _ in order:
                    copies[step, offset].start()

        for copy in copies.values():
            copy.wait_recv()
        for copy in copies.values():
            copy.wait_send()


def place_kernel(
    keys_ref, values_ref, scale_ref, out_keys, out_values, out_scale, after_ref, sem
):
    part = keys_ref.shape[0] // WRITES
    copies = [
        pltpu.make_async_copy(scale_ref, dst, sem.at[2, i]) for i, dst in enumerate((out_scale, after_ref))
    ]
    for i, (src, dst) in enumerate(((keys_ref, out_keys), (values_ref, out_values))):
        for j in range(WRITES):
            place = pl.ds(j * part, part)
            copies.append(pltpu.make_async_copy(src.at[place], dst.at[place], sem.at[i, j]))
    for copy in copies:
        copy.start()
    for copy in copies:
        copy.wait()


def place_tail_kernel(far_size, near_size, rows, values_ref, late_ref, out_ref, sem):
    me = position(near_size)

    @pl.when(me % 2 == 0)
    def _():
        copies, place = [], 0
        for i, (step, offset, size) in enumerate(exchange_plan(far_size, near_size, rows)[2]):
            copies.append(
                pltpu.make_async_copy(
                    late_ref.at[pl.ds(place, size)],
                    out_ref.at[pl.ds((me ^ step) * rows + offset, size)],
                    sem.at[i],
                )
            )
            place += size
        for copy in copies:
            copy.start()
        for copy in copies:
            copy.wait()


def local(far_size, near_size, raw_keys, raw_values, turn_angle, key_gain):
    sequences, positions, heads, size = raw_keys.shape
    devices = far_size * near_size
    rows = positions * heads
    total = rows * devices
    flat = (sequences, rows, size)
    even, odd, tail = exchange_plan(far_size, near_size, rows)
    raw_values = raw_values.reshape(flat)
    whole = pltpu.VMEM((total, size), raw_keys.dtype)
    keys, values, scale = pl.pallas_call(
        functools.partial(exchange_kernel, far_size, near_size, heads),
        out_shape=(whole, whole, pltpu.VMEM((heads, size), jnp.float32)),
        in_specs=[
            pl.BlockSpec(memory_space=pl.ANY),
            pl.BlockSpec(memory_space=pl.ANY),
            pl.BlockSpec(memory_space=pl.ANY),
            pl.BlockSpec(memory_space=pl.ANY),
        ],
        out_specs=(
            pl.BlockSpec(memory_space=pltpu.VMEM),
            pl.BlockSpec(memory_space=pltpu.VMEM),
            pl.BlockSpec(memory_space=pltpu.VMEM),
        ),
        scratch_shapes=[
            pltpu.VMEM((size // 2, total // heads), jnp.float32),
            pltpu.VMEM((1, size), jnp.float32),
            pltpu.VMEM((total, size), raw_keys.dtype),
            pltpu.VMEM((total, size), jnp.float32),
            pltpu.VMEM((total, size), jnp.float32),
            pltpu.VMEM((total, size), jnp.float32),
            pltpu.VMEM((RELAY, size), raw_keys.dtype),
            pltpu.SemaphoreType.DMA((len(set(even + odd)),)),
            pltpu.SemaphoreType.DMA((len(set(even + odd)),)),
            pltpu.SemaphoreType.DMA((3,)),
            pltpu.SemaphoreType.REGULAR((devices,)),
            pltpu.SemaphoreType.DMA((4,)),
        ],
        compiler_params=pltpu.CompilerParams(
            collective_id=0, has_side_effects=True, vmem_limit_bytes=48 * 1024 * 1024
        ),
        name="exchange",
    )(raw_keys.reshape(flat), raw_values, turn_angle.T, key_gain.reshape(1, size))
    out = jax.ShapeDtypeStruct((total, size), raw_keys.dtype)
    in_vmem = pl.BlockSpec(memory_space=pltpu.VMEM)
    anywhere = pl.BlockSpec(memory_space=pl.ANY)
    keys, values, scale, after = pl.pallas_call(
        place_kernel,
        out_shape=(
            out, out, jax.ShapeDtypeStruct((heads, size), jnp.float32),
            jax.ShapeDtypeStruct((heads, size), jnp.float32),
        ),
        in_specs=[in_vmem] * 3,
        out_specs=[anywhere] * 4,
        scratch_shapes=[pltpu.SemaphoreType.DMA((3, WRITES))],
        compiler_params=pltpu.CompilerParams(vmem_limit_bytes=12 * 1024 * 1024),
        name="place",
    )(keys, values, scale)
    late = pl.pallas_call(
        functools.partial(tail_kernel, far_size, near_size),
        out_shape=pltpu.VMEM((sum(copy[2] for copy in tail), size), raw_keys.dtype),
        in_specs=[anywhere, anywhere],
        out_specs=in_vmem,
        scratch_shapes=[pltpu.SemaphoreType.DMA((len(tail),))] * 2,
        compiler_params=pltpu.CompilerParams(
            collective_id=1, has_side_effects=True, vmem_limit_bytes=TAIL_VMEM
        ),
        name="tail",
    )(raw_values, after)
    values = pl.pallas_call(
        functools.partial(place_tail_kernel, far_size, near_size, rows),
        out_shape=out,
        in_specs=[anywhere, in_vmem],
        out_specs=anywhere,
        input_output_aliases={0: 0},
        scratch_shapes=[pltpu.SemaphoreType.DMA((len(tail),))],
        compiler_params=pltpu.CompilerParams(vmem_limit_bytes=12 * 1024 * 1024),
        name="place_tail",
    )(values, late)
    full = (1, positions * devices, heads, size)
    return keys.reshape(full), values.reshape(full), scale.reshape(1, heads, size)


def solution(mesh):
    in_specs = (
        P(None, (FAR, NEAR), "model", None),
        P(None, (FAR, NEAR), "model", None),
        P(),
        P(),
    )
    out_specs = (
        P((FAR, NEAR), None, "model", None),
        P((FAR, NEAR), None, "model", None),
        P((FAR, NEAR), "model", None),
    )
    body = functools.partial(local, mesh.shape[FAR], mesh.shape[NEAR])
    return jax.shard_map(body, mesh=mesh, in_specs=in_specs, out_specs=out_specs, check_vma=False)
```
